512 devices in a mesh: gx: 8 (over z_hi, core), gyz: 64 (over y, x, z_lo).
Axes of the slice: x: 4, y: 8, z: 8 (z_hi: 4, z_lo: 2; z = z_hi * 2 + z_lo), core: 2. Of those that a mesh axis runs over, the one named last changes fastest.
Arguments:
- bands: bfloat16 [64, 320, 40, 512], P('gx', 'gyz'), may hold values from -16 to 16
- potential: float32 [64, 320, 40], P('gx', 'gyz'), may hold values from 0.5 to 4
- eigenvectors: bfloat16 [512, 512], P('gyz'), may hold values from -0.25 to 0.25
Outputs:
- correlation: float32 [512, 512], P('gyz')
- hamiltonian: float32 [512, 512], P('gyz')
- rotated: bfloat16 [64, 320, 40, 512], P('gx', 'gyz')
The draws below stay inside these ranges and needn't reach their ends.
All inputs are finite; a program needn't handle non-finite values.
Results may differ from the reference program's by a relative error of at most 0.0012.
Values may be sent and summed in bfloat16 or wider, within the bound.
No kernel may reach another device: no remote copies, remote signals or barrier semaphores. Data moves between devices by JAX's collectives and lax.ppermute only.
A program may use at most 64 MiB of HBM per device.

```python
import math
import jax
import jax.numpy as jnp
from jax import lax

BANDS = 512
CX = 8
CZ = 40
NX = 64
NY = 320


def strengthened(drawn, stream_key, source, target, blocks, factor):
    def block_of(dim):
        return (jnp.arange(drawn.shape[dim]) // (drawn.shape[dim] // blocks)).reshape((-1,) + (1,) * (drawn.ndim - 1 - dim))

    one_side = jax.random.permutation(stream_key, blocks)[block_of(target)]
    other_side = (block_of(target) + blocks // 2) % blocks
    return jnp.where((block_of(source) == one_side) | (block_of(source) == other_side), factor * drawn, drawn)


def levels(rng, dims, pieces, least, largest):
    def one(position, blocks):
        heights = jax.random.uniform(jax.random.fold_in(jax.random.fold_in(rng, 6), position), (blocks,), jnp.float32, least / len(pieces), largest / len(pieces))
        return jnp.repeat(jnp.exp(heights), dims[position] // blocks).reshape((-1,) + (1,) * (len(dims) - position - 1))

    factor_of = one(*pieces[0])
    for cut in pieces[1:]:
        factor_of = factor_of * one(*cut)
    return factor_of


def normal_values(rng, extent, scale, reach, shards=(), held_as=jnp.bfloat16):
    result = jax.random.normal(rng, extent, jnp.float32) * scale
    if len(shards) > 0:
        result = levels(rng, extent, shards, -0.22, 0.18) * result
    return jnp.clip(result, min=-reach, max=reach).astype(held_as)


def bell_draw_with(key, extent, width, bound, pieces, heavy, held_as=jnp.bfloat16):
    entries = width * jax.random.normal(key, extent, jnp.float32)
    if pieces:
        entries = entries * levels(key, extent, pieces, -0.22, 0.18)
    return jnp.clip(strengthened(entries, jax.random.fold_in(key, 3), *heavy), -bound, bound).astype(held_as)


def setup_inputs(seed: int = 0) -> dict:
    streams_of = jax.random.split(jax.random.key(seed), 4)
    bands = bell_draw_with(streams_of[0], (NX, NY, CZ, BANDS), 1.0, 16.0, ((0, 8), (1, 64)), (1, 3, 64, 4.0))
    potential = jnp.clip(jnp.exp(math.log(4.0) - 2.0794415 * jax.random.uniform(streams_of[1], (NX, NY, CZ), jnp.float32) ** levels(streams_of[1], (NX, NY, CZ), ((0, 8), (1, 64)), -0.2, 0.2)), 0.5, 4.0)
    eigenvectors = normal_values(streams_of[2], (BANDS, BANDS), BANDS ** -0.5, 0.25, ((0, 64),))
    return dict(bands=bands, potential=potential, eigenvectors=eigenvectors)


def stencil(padded, potential):
    centre = padded[1:-1, 1:-1, 1:-1].astype(jnp.float32)
    neighbours = padded[2:, 1:-1, 1:-1].astype(jnp.float32) + padded[:-2, 1:-1, 1:-1].astype(jnp.float32)
    neighbours = neighbours + padded[1:-1, 2:, 1:-1].astype(jnp.float32) + padded[1:-1, :-2, 1:-1].astype(jnp.float32)
    neighbours = neighbours + padded[1:-1, 1:-1, 2:].astype(jnp.float32) + padded[1:-1, 1:-1, :-2].astype(jnp.float32)
    return ((3.0 + potential[..., None]) * centre - 0.5 * neighbours).astype(jnp.bfloat16)


def reference(bands, potential, eigenvectors):
    padded = jnp.pad(bands, ((1, 1), (1, 1), (1, 1), (0, 0)))

    def x_plane(plane_index):
        x_slab = lax.dynamic_slice_in_dim(padded, plane_index, 3, 0)
        local_pot = lax.dynamic_slice_in_dim(potential, plane_index, 1, 0)
        return stencil(x_slab, local_pot)[0]

    hamil_bands = lax.map(x_plane, jnp.arange(NX, dtype=jnp.int32))
    cell_count = NX * NY * CZ
    flat_bands = bands.reshape(cell_count, BANDS)
    flat_hamil = hamil_bands.reshape(cell_count, BANDS)
    inv_volume = 1.0 / (CX * NY * CZ)
    correlation = lax.dot_general(flat_bands, flat_bands, (((0,), (0,)), ((), ())), preferred_element_type=jnp.float32) * inv_volume
    hamiltonian = lax.dot_general(flat_bands, flat_hamil, (((0,), (0,)), ((), ())), preferred_element_type=jnp.float32) * inv_volume
    rotated = jnp.dot(flat_bands, eigenvectors, preferred_element_type=jnp.float32).astype(jnp.bfloat16)
    return correlation, hamiltonian, rotated.reshape(bands.shape)
```

```python
import functools

import jax
import jax.numpy as jnp
from jax import lax
from jax.experimental import pallas as pl
from jax.experimental.pallas import tpu as pltpu
from jax.sharding import PartitionSpec as P


F32 = jnp.float32
BF16 = jnp.bfloat16


def over_rows(a, b):
    return lax.dot_general(a, b, (((0,), (0,)), ((), ())), preferred_element_type=F32)


def stencil_kernel(bands_ref, pot_ref, out_ref):
    nx, ny, nz, nb = bands_ref.shape
    row = lax.broadcasted_iota(jnp.int32, (nz, nb), 0)

    def plane(x, carry):
        below = jnp.where(x > 0, 0.5, 0.0)
        above = jnp.where(x < nx - 1, 0.5, 0.0)
        pot = jnp.transpose(pot_ref[x])
        tiles = [bands_ref[x, y].astype(F32) for y in range(ny)]
        for y in range(ny):
            centre = tiles[y]
            total = jnp.where(row > 0, pltpu.roll(centre, 1, 0), 0.0)
            total += jnp.where(row < nz - 1, pltpu.roll(centre, nz - 1, 0), 0.0)
            if y > 0:
                total += tiles[y - 1]
            if y < ny - 1:
                total += tiles[y + 1]
            low = bands_ref[jnp.maximum(x - 1, 0), y].astype(F32)
            high = bands_ref[jnp.minimum(x + 1, nx - 1), y].astype(F32)
            value = (3.0 + pot[:, y : y + 1]) * centre - 0.5 * total
            value -= below * low + above * high
            out_ref[x, y] = value.astype(BF16)
        return carry

    lax.fori_loop(0, nx, plane, 0)


def local_stencil(bands, potential):
    return pl.pallas_call(
        stencil_kernel,
        out_shape=jax.ShapeDtypeStruct(bands.shape, BF16),
        in_specs=[pl.BlockSpec(memory_space=pltpu.VMEM)] * 2,
        out_specs=pl.BlockSpec(memory_space=pltpu.VMEM),
        cost_estimate=pl.CostEstimate(
            flops=12 * bands.size, bytes_accessed=4 * bands.size, transcendentals=0
        ),
        compiler_params=pltpu.CompilerParams(vmem_limit_bytes=12 << 20),
        name="stencil",
    )(bands, potential)


def cross_kernel(scale, local_ref, first_ref, slab_ref, yhalo_ref, xhalo_ref, out_ref):
    nb = local_ref.shape[0]
    first = first_ref[...].reshape(-1, nb)
    slab = slab_ref[...].reshape(-1, nb)
    yhalo = yhalo_ref[...].reshape(-1, nb)
    xhalo = xhalo_ref[...].reshape(-1, nb)
    cross = over_rows(first, yhalo) + over_rows(slab, xhalo)
    cross += over_rows(yhalo, first) + over_rows(xhalo, slab)
    out_ref[...] = (scale * (local_ref[...] - 0.5 * cross)).astype(BF16)


def add_cross(scale, local, first, slab, yhalo, xhalo):
    nb = local.shape[0]
    rows = first.size // nb + slab.size // nb
    return pl.pallas_call(
        functools.partial(cross_kernel, scale),
        out_shape=jax.ShapeDtypeStruct(local.shape, BF16),
        in_specs=[pl.BlockSpec(memory_space=pltpu.VMEM)] * 5,
        out_specs=pl.BlockSpec(memory_space=pltpu.VMEM),
        cost_estimate=pl.CostEstimate(
            flops=4 * rows * nb * nb, bytes_accessed=6 * nb * nb, transcendentals=0
        ),
        compiler_params=pltpu.CompilerParams(vmem_limit_bytes=12 << 20),
        name="cross",
    )(local, first, slab, yhalo, xhalo)


def x_pairs(gx, gyz):
    pairs = []
    for r in range(gyz):
        for g in range(gx - 1):
            low, high = g * gyz + r, (g + 1) * gyz + r
            pairs.append((low, high) if r % 2 == 0 else (high, low))
    return pairs


def to_rows(x, axis):
    count = lax.axis_size(axis)
    parts = x.reshape(count, x.shape[0] // count, x.shape[1])
    return lax.all_to_all(parts, axis, 0, 0, tiled=True)


def from_everyone(x, axis):
    count = lax.axis_size(axis)
    return lax.all_to_all(jnp.broadcast_to(x[None], (count, *x.shape)), axis, 0, 0, tiled=True)


def projected(bands, potential, eigenvectors):
    nx, ny, nz, nb = bands.shape
    gx, gyz = lax.axis_size("gx"), lax.axis_size("gyz")
    odd = lax.rem(lax.axis_index("gyz"), 2)
    cells = nx * ny * nz
    scale = 1.0 / (cells * gyz)
    flat = bands.reshape(cells, nb)

    sent_slab = jnp.where(odd == 0, nx - 1, 0)
    last = lax.slice_in_dim(bands, ny - 1, ny, axis=1)
    slab = lax.dynamic_slice_in_dim(bands, sent_slab, 1, axis=0)
    yhalo = lax.ppermute(last, "gyz", [(i, i + 1) for i in range(gyz - 1)])
    xhalo = lax.ppermute(slab, ("gx", "gyz"), x_pairs(gx, gyz))

    corr = (over_rows(flat, flat) * scale).astype(BF16)
    corr_parts = to_rows(corr, "gyz")

    hamil_bands = local_stencil(bands, potential)
    local = over_rows(flat, hamil_bands.reshape(cells, nb))
    first = lax.slice_in_dim(bands, 0, 1, axis=1)
    own_slab = lax.dynamic_slice_in_dim(bands, nx - 1 - sent_slab, 1, axis=0)
    hamil = add_cross(scale, local, first, own_slab, yhalo, xhalo)
    hamil_parts = to_rows(hamil, "gyz")

    coefficients = from_everyone(eigenvectors, "gyz").reshape(nb, nb)
    rotated = jnp.dot(flat, coefficients, preferred_element_type=F32).astype(BF16)

    rows = jnp.concatenate(
        (corr_parts.astype(F32).sum(axis=0), hamil_parts.astype(F32).sum(axis=0)), axis=1
    )
    total = from_everyone(rows, "gx").sum(axis=0)
    return total[:, :nb], total[:, nb:], rotated.reshape(bands.shape)


def solution(mesh):
    in_specs = (P("gx", "gyz", None, None), P("gx", "gyz", None), P("gyz", None))
    out_specs = (P("gyz", None), P("gyz", None), P("gx", "gyz", None, None))
    return jax.shard_map(
        projected, mesh=mesh, in_specs=in_specs, out_specs=out_specs, check_vma=False
    )
```

```python
import functools

import jax
import jax.numpy as jnp
from jax import lax
from jax.experimental import pallas as pl
from jax.experimental.pallas import tpu as pltpu
from jax.sharding import PartitionSpec as P


F32 = jnp.float32
BF16 = jnp.bfloat16
BOTH = ("gx", "gyz")


def over_rows(a, b):
    return lax.dot_general(a, b, (((0,), (0,)), ((), ())), preferred_element_type=F32)


def half_stencil(core, planes, pots, outs):
    nx, ny, nz, nb = planes[0].shape
    row = lax.broadcasted_iota(jnp.int32, (nz, nb), 0)
    half = jnp.where(core == 1, 0.5, 0.0).astype(F32)

    def tiles_at(ref, x):
        return [ref[x, y].astype(F32) for y in range(ny)]

    def one(ref, pot_ref, out_ref, x, below, weight):
        pot = jnp.transpose(pot_ref[x])
        factor = 0.5 + half * (2.0 + pot)
        tiles = tiles_at(ref, x)
        for y in range(ny):
            total = jnp.where(row > 0, pltpu.roll(tiles[y], 1, 0), 0.0)
            if y > 0:
                total += tiles[y - 1]
            value = factor[:, y : y + 1] * tiles[y] - half * total - weight * below[y]
            out_ref[x, y] = value.astype(BF16)

    low, high = planes
    zero = [jnp.zeros((nz, nb), F32)] * ny
    one(low, pots[0], outs[0], 0, zero, half)
    one(high, pots[1], outs[1], 0, tiles_at(low, nx - 1), half)

    def step(x, carry):
        for ref, pot, out in zip(planes, pots, outs):
            one(ref, pot, out, x, tiles_at(ref, x - 1), half)
        return carry

    lax.fori_loop(1, nx, step, 0)


def gram_kernel(
    scale, place_ref, own_ref, other_ref, pot_ref, other_pot_ref, yown_ref, yother_ref, xhalo_ref,
    out_ref, right_own, right_other,
):
    nx, _, _, nb = own_ref.shape
    core, odd = place_ref[0], place_ref[1]
    half_stencil(
        core, (other_ref, own_ref), (other_pot_ref, pot_ref), (right_other, right_own)
    )

    def rows(value):
        return value.reshape(-1, nb)

    gram = over_rows(rows(own_ref[...]), rows(right_own[...]))
    gram += over_rows(rows(other_ref[...]), rows(right_other[...]))
    cross = over_rows(rows(own_ref[:, 0]), rows(yown_ref[...]))
    cross += over_rows(rows(other_ref[:, 0]), rows(yother_ref[...]))
    slab = jnp.where(odd == 0, other_ref[0], own_ref[nx - 1])
    cross += over_rows(rows(slab), rows(xhalo_ref[...]))
    gram -= 0.5 * cross
    out_ref[...] = (scale * (gram + jnp.transpose(gram))).astype(BF16)


def gram_partial(scale, place, own, other, pot, other_pot, yown, yother, xhalo):
    nb = own.shape[-1]
    rows = 2 * (own.size // nb)
    vmem = pl.BlockSpec(memory_space=pltpu.VMEM)
    return pl.pallas_call(
        functools.partial(gram_kernel, scale),
        out_shape=jax.ShapeDtypeStruct((nb, nb), BF16),
        in_specs=[pl.BlockSpec(memory_space=pltpu.SMEM)] + [vmem] * 7,
        out_specs=vmem,
        scratch_shapes=[pltpu.VMEM(own.shape, BF16)] * 2,
        cost_estimate=pl.CostEstimate(
            flops=2 * rows * nb * nb, bytes_accessed=4 * rows * nb, transcendentals=0
        ),
        compiler_params=pltpu.CompilerParams(vmem_limit_bytes=24 << 20),
        name="gram",
    )(place, own, other, pot, other_pot, yown, yother, xhalo)


def pairs_of(gx, gyz):
    def at(g, r):
        return g * gyz + r

    same, next_core, x = [], [], []
    for chip in range(gx // 2):
        for r in range(gyz - 1):
            same.append((at(2 * chip + 1, r), at(2 * chip + 1, r + 1)))
            next_core.append((at(2 * chip, r), at(2 * chip + 1, r + 1)))
    for chip in range(gx // 2 - 1):
        for r in range(gyz):
            if r % 2 == 0:
                x.append((at(2 * chip + 1, r), at(2 * chip + 3, r)))
            else:
                x.append((at(2 * chip + 2, r), at(2 * chip + 1, r)))
    return same, next_core, x


def to_rows(x, axis):
    count = lax.axis_size(axis)
    parts = x.reshape(count, x.shape[0] // count, x.shape[1])
    return lax.all_to_all(parts, axis, 0, 0, tiled=True)


def from_everyone(x, axis):
    count = lax.axis_size(axis)
    return lax.all_to_all(jnp.broadcast_to(x[None], (count, *x.shape)), axis, 0, 0, tiled=True)


def projected(bands, potential, eigenvectors):
    nx, ny, nz, nb = bands.shape
    gx, gyz = lax.axis_size("gx"), lax.axis_size("gyz")
    core = lax.rem(lax.axis_index("gx"), 2)
    odd = lax.rem(lax.axis_index("gyz"), 2)
    cells = nx * ny * nz
    scale = 1.0 / (cells * gyz)

    same, next_core, x_pairs = pairs_of(gx, gyz)
    partner = [(g, g ^ 1) for g in range(gx)]
    last = lax.slice_in_dim(bands, ny - 1, ny, axis=1)
    slab = lax.dynamic_slice_in_dim(bands, jnp.where(odd == 0, nx - 1, 0), 1, axis=0)
    yother = lax.ppermute(last, BOTH, next_core)
    yown = lax.ppermute(last, BOTH, same)
    xhalo = lax.ppermute(slab, BOTH, x_pairs)
    other = lax.ppermute(bands, "gx", partner)
    other_pot = lax.ppermute(potential, "gx", partner)

    coefficients = from_everyone(eigenvectors, "gyz").reshape(nb, nb)

    place = jnp.stack((core, odd)).astype(jnp.int32)
    gram = gram_partial(
        scale, place, bands, other, potential, other_pot, yown, yother, xhalo
    )
    gram_parts = to_rows(gram, "gyz")
    rotated = jnp.dot(
        bands.reshape(cells, nb), coefficients, preferred_element_type=F32
    ).astype(BF16)

    parts = from_everyone(gram_parts.astype(F32).sum(axis=0), "gx")
    sums = parts.reshape(gx // 2, 2, *parts.shape[1:]).sum(axis=0)
    return sums[0], sums[1], rotated.reshape(bands.shape)


def solution(mesh):
    in_specs = (P("gx", "gyz", None, None), P("gx", "gyz", None), P("gyz", None))
    out_specs = (P("gyz", None), P("gyz", None), P("gx", "gyz", None, None))
    return jax.shard_map(
        projected, mesh=mesh, in_specs=in_specs, out_specs=out_specs, check_vma=False
    )
```

```python
import functools

import jax
import jax.numpy as jnp
from jax import lax
from jax.experimental import pallas as pl
from jax.experimental.pallas import tpu as pltpu
from jax.sharding import PartitionSpec as P


F32 = jnp.float32
BF16 = jnp.bfloat16
BOTH = ("gx", "gyz")
PIECES = 3

VMEM = pl.BlockSpec(memory_space=pltpu.VMEM)
SMEM = pl.BlockSpec(memory_space=pltpu.SMEM)


def over_rows(a, b):
    return lax.dot_general(a, b, (((0,), (0,)), ((), ())), preferred_element_type=F32)


def call(kernel, out_shape, in_specs, args, scratch=(), flops=0):
    many = isinstance(out_shape, tuple)
    moved = sum(a.size * a.dtype.itemsize for a in args)
    return pl.pallas_call(
        kernel,
        out_shape=out_shape,
        in_specs=in_specs,
        out_specs=(VMEM,) * len(out_shape) if many else VMEM,
        scratch_shapes=list(scratch),
        cost_estimate=pl.CostEstimate(flops=flops, bytes_accessed=moved, transcendentals=0),
        compiler_params=pltpu.CompilerParams(vmem_limit_bytes=20 << 20),
    )(*args)


def prepare_kernel(place_ref, bands_ref, pot_ref, held_ref, last_ref, slab_ref, sems):
    nx, ny, nz, _ = bands_ref.shape
    sent = jnp.where(place_ref[1] == 0, nx - 1, 0)
    copies = (
        pltpu.make_async_copy(bands_ref.at[:, ny - 1], last_ref, sems.at[0]),
        pltpu.make_async_copy(bands_ref.at[sent], slab_ref, sems.at[1]),
        pltpu.make_async_copy(bands_ref, held_ref.at[pl.ds(0, nx)], sems.at[2]),
    )
    for copy in copies:
        copy.start()
    rest = pot_ref[...].reshape(nx * ny, nz)
    for piece in range(PIECES):
        part = rest.astype(BF16)
        held_ref[nx, piece, 0 : nx * ny, 0:nz] = part
        rest = rest - part.astype(F32)
    for copy in copies:
        copy.wait()


def prepare(place, bands, pot):
    nx, ny, nz, nb = bands.shape
    assert ny >= PIECES and nx * ny <= nz <= nb
    shapes = ((nx + 1, ny, nz, nb), (nx, nz, nb), (ny, nz, nb))
    return call(
        prepare_kernel,
        tuple(jax.ShapeDtypeStruct(s, BF16) for s in shapes),
        [SMEM, pl.BlockSpec(memory_space=pltpu.HBM), VMEM],
        (place, bands, pot),
        scratch=[pltpu.SemaphoreType.DMA((3,))],
    )


def half_stencil(core, planes, pots, outs):
    nx, ny, nz, nb = outs[0].shape
    row = lax.broadcasted_iota(jnp.int32, (nz, nb), 0)
    half = jnp.where(core == 1, 0.5, 0.0).astype(F32)

    def tiles_at(ref, x):
        return [ref[x, y].astype(F32) for y in range(ny)]

    def one(ref, pot_ref, out_ref, x, below):
        pot = jnp.transpose(pot_ref[:, pl.ds(x, 1), :].reshape(ny, nz))
        factor = 0.5 + half * (2.0 + pot)
        tiles = tiles_at(ref, x)
        for y in range(ny):
            total = jnp.where(row > 0, pltpu.roll(tiles[y], 1, 0), 0.0)
            if y > 0:
                total += tiles[y - 1]
            if below is not None:
                total += below[y]
            out_ref[x, y] = (factor[:, y : y + 1] * tiles[y] - half * total).astype(BF16)

    low, high = planes
    one(low, pots[0], outs[0], 0, None)
    one(high, pots[1], outs[1], 0, tiles_at(low, nx - 1))

    def step(x, carry):
        for ref, pot, out in zip(planes, pots, outs):
            one(ref, pot, out, x, tiles_at(ref, x - 1))
        return carry

    lax.fori_loop(1, nx, step, 0)


def local_kernel(place_ref, own_ref, other_ref, pot_ref, gram_ref, other_pot, right_own, right_other):
    nx, ny, nz, nb = right_own.shape
    pieces = [other_ref[nx, p, 0 : nx * ny, 0:nz].astype(F32) for p in range(PIECES)]
    other_pot[...] = ((pieces[2] + pieces[1]) + pieces[0]).reshape(ny, nx, nz)
    half_stencil(
        place_ref[0], (other_ref, own_ref), (other_pot, pot_ref), (right_other, right_own)
    )

    def rows(ref):
        return ref[0:nx].reshape(-1, nb)

    gram_ref[...] = over_rows(rows(own_ref), rows(right_own)) + over_rows(
        rows(other_ref), rows(right_other)
    )


def local_gram(place, own, other, pot, shape):
    nx, ny, nz, nb = shape
    return call(
        local_kernel,
        jax.ShapeDtypeStruct((nb, nb), F32),
        [SMEM, VMEM, VMEM, VMEM],
        (place, own, other, pot),
        scratch=[pltpu.VMEM(pot.shape, F32)] + [pltpu.VMEM(shape, BF16)] * 2,
        flops=4 * nx * ny * nz * nb * nb,
    )


def cross_kernel(
    scale, place_ref, gram_ref, own_ref, other_ref, yown_ref, yother_ref, xhalo_ref, coef_ref, out_ref
):
    _, _, nb = xhalo_ref.shape
    nx = yown_ref.shape[0]
    groups, depth = out_ref.shape[0], coef_ref.shape[0]

    def rows(value):
        return value.reshape(-1, nb)

    cross = over_rows(rows(own_ref[0:nx, 0]), rows(yown_ref[...]))
    cross += over_rows(rows(other_ref[0:nx, 0]), rows(yother_ref[...]))
    slab = jnp.where(place_ref[1] == 0, other_ref[0], own_ref[nx - 1])
    cross += over_rows(rows(slab), rows(xhalo_ref[...]))
    gram = gram_ref[...] - 0.5 * cross
    total = (scale * (gram + jnp.transpose(gram))).astype(BF16)
    total = total.reshape(nb // (groups * depth), groups, depth, nb)
    for d in range(groups):
        out_ref[d, 0 : nb // groups] = rows(total[:, d])
        out_ref[d, nb // groups :] = coef_ref[...]


def add_cross(scale, groups, place, gram, own, other, yown, yother, xhalo, coef):
    nb = gram.shape[0]
    depth = coef.shape[0]
    halo_rows = (yown.size + yother.size + xhalo.size) // nb
    return call(
        functools.partial(cross_kernel, scale),
        jax.ShapeDtypeStruct((groups, nb // groups + depth, nb), BF16),
        [SMEM] + [VMEM] * 7,
        (place, gram, own, other, yown, yother, xhalo, coef),
        flops=2 * halo_rows * nb * nb,
    )


def middle_kernel(place_ref, in_ref, out_ref):
    sources, height, nb = in_ref.shape
    targets, _, _ = out_ref.shape
    depth = (height * targets - nb * targets // sources) // targets
    width = nb // 2
    total = in_ref[0, 0 : height - depth].astype(F32)
    for s in range(1, sources):
        total += in_ref[s, 0 : height - depth].astype(F32)
    total = total.astype(BF16).reshape(targets, depth, nb)
    upper = sources // 2
    for s in range(sources):
        coef = in_ref[s, height - depth :]
        coef = jnp.where(place_ref[0] == 0, coef[:, :width], coef[:, width:])
        first = depth + (s % upper) * depth
        lane = (s // upper) * width
        for t in range(targets):
            out_ref[t, first : first + depth, lane : lane + width] = coef
    for t in range(targets):
        out_ref[t, 0:depth] = total[t]


def middle(place, arrived, targets):
    sources, height, nb = arrived.shape
    depth = height - nb // sources
    return call(
        middle_kernel,
        jax.ShapeDtypeStruct((targets, depth + sources * depth // 2, nb), BF16),
        [SMEM, VMEM],
        (place, arrived),
    )


def last_kernel(in_ref, rows_ref, coef_ref):
    sources, height, nb = in_ref.shape
    copies, depth, _ = rows_ref.shape
    total = in_ref[0, 0:depth].astype(F32)
    for s in range(1, sources):
        total += in_ref[s, 0:depth].astype(F32)
    for c in range(copies):
        rows_ref[c] = total
    plane = 2 * (height - depth)
    for s in range(sources):
        for part in range(2):
            start = s * plane + part * (plane // 2)
            coef_ref[start : start + plane // 2] = in_ref[
                s, depth:, part * (nb // 2) : (part + 1) * (nb // 2)
            ]


def finish(arrived, copies, depth):
    _, _, nb = arrived.shape
    return call(
        last_kernel,
        (
            jax.ShapeDtypeStruct((copies, depth, nb), F32),
            jax.ShapeDtypeStruct((nb, nb // 2), BF16),
        ),
        [VMEM],
        (arrived,),
    )


def pairs_of(gx, gyz):
    def at(g, r):
        return g * gyz + r

    same, next_core, x = [], [], []
    for chip in range(gx // 2):
        for r in range(gyz - 1):
            same.append((at(2 * chip + 1, r), at(2 * chip + 1, r + 1)))
            next_core.append((at(2 * chip, r), at(2 * chip + 1, r + 1)))
    for chip in range(gx // 2 - 1):
        for r in range(gyz):
            if r % 2 == 0:
                x.append((at(2 * chip + 1, r), at(2 * chip + 3, r)))
            else:
                x.append((at(2 * chip + 2, r), at(2 * chip + 1, r)))
    return same, next_core, x


def exchanged(x, axis, groups=None):
    return lax.all_to_all(x, axis, 0, 0, tiled=True, axis_index_groups=groups)


def projected(bands, potential, eigenvectors):
    nx, ny, nz, nb = bands.shape
    gx, gyz = lax.axis_size("gx"), lax.axis_size("gyz")
    depth = eigenvectors.shape[0]
    inner = 8
    outer = gyz // inner
    core = lax.rem(lax.axis_index("gx"), 2)
    odd = lax.rem(lax.axis_index("gyz"), 2)
    cells = nx * ny * nz
    scale = 1.0 / (cells * gyz)
    place = jnp.stack((core, odd)).astype(jnp.int32)
    pot = jnp.transpose(potential, (1, 0, 2))

    own, last, slab = prepare(place, bands, pot)
    same, next_core, x_pairs = pairs_of(gx, gyz)
    partner = [(g, g ^ 1) for g in range(gx)]
    yother = lax.ppermute(last, BOTH, next_core)
    yown = lax.ppermute(last, BOTH, same)
    xhalo = lax.ppermute(slab, BOTH, x_pairs)
    other = lax.ppermute(own, "gx", partner)

    gram = local_gram(place, own, other, pot, bands.shape)
    sent = add_cross(
        scale, inner, place, gram, own, other, yown, yother, xhalo, eigenvectors
    )
    arrived = exchanged(sent, "gyz", [[o * inner + i for i in range(inner)] for o in range(outer)])
    sent = middle(place, arrived, outer)
    arrived = exchanged(sent, "gyz", [[o * inner + i for o in range(outer)] for i in range(inner)])
    rows, coef = finish(arrived, gx, depth)
    coef_other = lax.ppermute(coef, "gx", partner)
    parts = exchanged(rows, "gx")
    sums = parts.reshape(gx // 2, 2, *parts.shape[1:]).sum(axis=0)

    left = jnp.where(core == 0, coef, coef_other)
    right = jnp.where(core == 0, coef_other, coef)
    rotated = jnp.dot(
        bands.reshape(cells, nb),
        jnp.concatenate((left, right), axis=1),
        preferred_element_type=F32,
    ).astype(BF16)
    return sums[0], sums[1], rotated.reshape(bands.shape)


def solution(mesh):
    in_specs = (P("gx", "gyz", None, None), P("gx", "gyz", None), P("gyz", None))
    out_specs = (P("gyz", None), P("gyz", None), P("gx", "gyz", None, None))
    return jax.shard_map(
        projected, mesh=mesh, in_specs=in_specs, out_specs=out_specs, check_vma=False
    )
```

```python
import functools

import jax
import jax.numpy as jnp
from jax import lax
from jax.experimental import pallas as pl
from jax.experimental.pallas import tpu as pltpu
from jax.sharding import PartitionSpec as P


F32 = jnp.float32
BF16 = jnp.bfloat16
BOTH = ("gx", "gyz")
PIECES = 3

VMEM = pl.BlockSpec(memory_space=pltpu.VMEM)
SMEM = pl.BlockSpec(memory_space=pltpu.SMEM)


def over_rows(a, b):
    return lax.dot_general(a, b, (((0,), (0,)), ((), ())), preferred_element_type=F32)


def call(kernel, out_shape, in_specs, args, scratch=(), flops=0):
    many = isinstance(out_shape, tuple)
    moved = sum(a.size * a.dtype.itemsize for a in args)
    return pl.pallas_call(
        kernel,
        out_shape=out_shape,
        in_specs=in_specs,
        out_specs=(VMEM,) * len(out_shape) if many else VMEM,
        scratch_shapes=list(scratch),
        cost_estimate=pl.CostEstimate(flops=flops, bytes_accessed=moved, transcendentals=0),
        compiler_params=pltpu.CompilerParams(vmem_limit_bytes=20 << 20),
    )(*args)


def half_kernel(place_ref, bands_ref, pot_ref, *refs):
    nx, ny, nz, nb = bands_ref.shape
    right_ref, gram_ref = refs[-1], refs[-2]
    row = lax.broadcasted_iota(jnp.int32, (nz, nb), 0)
    half = jnp.where(place_ref[0] == 1, 0.5, 0.0).astype(F32)

    def slab(x, below):
        pot = jnp.transpose(pot_ref[:, pl.ds(x, 1), :].reshape(ny, nz))
        factor = 0.5 + half * (2.0 + pot)
        tiles = [bands_ref[x, y].astype(F32) for y in range(ny)]
        for y in range(ny):
            total = jnp.where(row > 0, pltpu.roll(tiles[y], 1, 0), 0.0)
            if y > 0:
                total += tiles[y - 1]
            if below is not None:
                total += below[y]
            right_ref[x, y] = (factor[:, y : y + 1] * tiles[y] - half * total).astype(BF16)
        return tiles

    lax.fori_loop(1, nx, lambda x, below: slab(x, below), slab(0, None))
    gram = over_rows(bands_ref[...].reshape(-1, nb), right_ref[...].reshape(-1, nb))
    if len(refs) > 2:
        gram += refs[0][...]
    gram_ref[...] = gram


def half_gram(place, bands, pot, given=()):
    nb = bands.shape[-1]
    return call(
        half_kernel,
        jax.ShapeDtypeStruct((nb, nb), F32),
        [SMEM] + [VMEM] * (2 + len(given)),
        (place, bands, pot, *given),
        scratch=[pltpu.VMEM(bands.shape, BF16)],
        flops=2 * bands.size * nb,
    )


def cross_kernel(
    scale, place_ref, gram_ref, own_ref, other_ref, yown_ref, yother_ref, xhalo_ref, coef_ref, out_ref
):
    _, _, nb = xhalo_ref.shape
    nx = yown_ref.shape[0]
    groups, depth = out_ref.shape[0], coef_ref.shape[0]

    def rows(value):
        return value.reshape(-1, nb)

    cross = over_rows(rows(own_ref[0:nx, 0]), rows(yown_ref[...]))
    cross += over_rows(rows(other_ref[0:nx, 0]), rows(yother_ref[...]))
    slab = jnp.where(place_ref[1] == 0, other_ref[0], own_ref[nx - 1])
    cross += over_rows(rows(slab), rows(xhalo_ref[...]))
    inside = over_rows(rows(own_ref[0]), rows(other_ref[nx - 1]))
    gram = gram_ref[...] - 0.5 * (cross + jnp.where(place_ref[0] == 1, inside, 0.0))
    total = (scale * (gram + jnp.transpose(gram))).astype(BF16)
    total = total.reshape(nb // (groups * depth), groups, depth, nb)
    for d in range(groups):
        out_ref[d, 0 : nb // groups] = rows(total[:, d])
        out_ref[d, nb // groups :] = coef_ref[...]


def add_cross(scale, groups, place, gram, own, other, yown, yother, xhalo, coef):
    nb = gram.shape[0]
    depth = coef.shape[0]
    halo_rows = (yown.size + yother.size + xhalo.size) // nb
    return call(
        functools.partial(cross_kernel, scale),
        jax.ShapeDtypeStruct((groups, nb // groups + depth, nb), BF16),
        [SMEM] + [VMEM] * 7,
        (place, gram, own, other, yown, yother, xhalo, coef),
        flops=2 * halo_rows * nb * nb,
    )


def middle_kernel(place_ref, in_ref, out_ref):
    core, chip = place_ref[0], place_ref[2]
    sources, height, nb = in_ref.shape
    rows = nb // sources
    depth = height - rows
    targets = rows // depth
    copies = out_ref.shape[0] // targets
    width = nb // 2
    total = in_ref[0, 0:rows].astype(F32)
    for s in range(1, sources):
        total += in_ref[s, 0:rows].astype(F32)
    total = total.astype(BF16).reshape(targets, depth, nb)
    share = sources // copies
    coef = [in_ref[share * chip + i, rows:] for i in range(share)]
    coef = jnp.concatenate(
        [jnp.where(core == 0, c[:, :width], c[:, width:]) for c in coef], axis=1
    )
    for t in range(targets):
        for c in range(copies):
            out_ref[t * copies + c, 0:depth] = total[t]
            out_ref[t * copies + c, depth:] = coef


def middle(place, arrived, targets, copies):
    sources, height, nb = arrived.shape
    depth = height - nb // sources
    assert sources == 2 * copies and targets * depth == nb // sources
    return call(
        middle_kernel,
        jax.ShapeDtypeStruct((targets * copies, 2 * depth, nb), BF16),
        [SMEM, VMEM],
        (place, arrived),
    )


def finish_kernel(in_ref, rows_ref, sent_ref):
    sources, height, nb = in_ref.shape
    depth, width = height // 2, nb // 2
    total = in_ref[0, 0:depth].astype(F32)
    for s in range(1, sources):
        total += in_ref[s, 0:depth].astype(F32)
    rows_ref[...] = total
    for s in range(sources):
        for part in range(2):
            start = (2 * s + part) * depth
            sent_ref[start : start + depth] = in_ref[
                s, depth:, part * width : (part + 1) * width
            ]
    for piece in range(PIECES):
        value = total.astype(BF16)
        total = total - value.astype(F32)
        for part in range(2):
            start = nb + (2 * piece + part) * depth
            sent_ref[start : start + depth] = value[:, part * width : (part + 1) * width]


def finish(arrived):
    _, height, nb = arrived.shape
    depth = height // 2
    return call(
        finish_kernel,
        (
            jax.ShapeDtypeStruct((depth, nb), F32),
            jax.ShapeDtypeStruct((nb + 2 * PIECES * depth, nb // 2), BF16),
        ),
        [VMEM],
        (arrived,),
    )


def rotate_kernel(place_ref, bands_ref, rows_ref, mine_ref, theirs_ref, corr_ref, hamil_ref, out_ref):
    core = place_ref[0]
    depth, nb = rows_ref.shape
    width = nb // 2
    block = out_ref.shape[0]
    step = pl.program_id(0)
    left = jnp.where(core == 0, mine_ref[0:nb], theirs_ref[0:nb])
    right = jnp.where(core == 0, theirs_ref[0:nb], mine_ref[0:nb])
    some = bands_ref[pl.ds(pl.multiple_of(step * block, block), block)]
    out_ref[:, :width] = jnp.dot(some, left, preferred_element_type=F32).astype(BF16)
    out_ref[:, width:] = jnp.dot(some, right, preferred_element_type=F32).astype(BF16)

    @pl.when(step == 0)
    def _():
        halves = []
        for part in range(2):
            starts = [nb + (2 * piece + part) * depth for piece in range(PIECES)]
            parts = [theirs_ref[s : s + depth].astype(F32) for s in starts]
            halves.append((parts[2] + parts[1]) + parts[0])
        theirs = jnp.concatenate(halves, axis=1)
        mine = rows_ref[...]
        corr_ref[...] = jnp.where(core == 0, mine, theirs)
        hamil_ref[...] = jnp.where(core == 0, theirs, mine)


def rotate(place, flat, rows, mine, theirs):
    cells, nb = flat.shape
    depth = rows.shape[0]
    steps = 5
    block = cells // steps
    small = pl.BlockSpec((depth, nb), lambda i: (0, 0))
    return pl.pallas_call(
        rotate_kernel,
        grid=(steps,),
        out_shape=(
            jax.ShapeDtypeStruct((depth, nb), F32),
            jax.ShapeDtypeStruct((depth, nb), F32),
            jax.ShapeDtypeStruct((cells, nb), BF16),
        ),
        in_specs=[SMEM] + [VMEM] * 4,
        out_specs=(small, small, pl.BlockSpec((block, nb), lambda i: (i, 0))),
        cost_estimate=pl.CostEstimate(
            flops=2 * cells * nb * nb, bytes_accessed=4 * cells * nb, transcendentals=0
        ),
        compiler_params=pltpu.CompilerParams(vmem_limit_bytes=20 << 20),
        name="rotate",
    )(place, flat, rows, mine, theirs)


def pairs_of(gx, gyz):
    def at(g, r):
        return g * gyz + r

    same, next_core, x = [], [], []
    for chip in range(gx // 2):
        for r in range(gyz - 1):
            same.append((at(2 * chip + 1, r), at(2 * chip + 1, r + 1)))
            next_core.append((at(2 * chip, r), at(2 * chip + 1, r + 1)))
    for chip in range(gx // 2 - 1):
        for r in range(gyz):
            if r % 2 == 0:
                x.append((at(2 * chip + 1, r), at(2 * chip + 3, r)))
            else:
                x.append((at(2 * chip + 2, r), at(2 * chip + 1, r)))
    return same, next_core, x


def exchanged(x, axis, groups=None):
    return lax.all_to_all(x, axis, 0, 0, tiled=True, axis_index_groups=groups)


def projected(bands, potential, eigenvectors):
    nx, ny, nz, nb = bands.shape
    gx, gyz = lax.axis_size("gx"), lax.axis_size("gyz")
    inner = 8
    outer = gyz // inner
    core = lax.rem(lax.axis_index("gx"), 2)
    odd = lax.rem(lax.axis_index("gyz"), 2)
    cells = nx * ny * nz
    scale = 1.0 / (cells * gyz)
    chip = lax.axis_index("gx") // 2
    place = jnp.stack((core, odd, chip)).astype(jnp.int32)
    pot = jnp.transpose(potential, (1, 0, 2))

    same, next_core, x_pairs = pairs_of(gx, gyz)
    partner = [(g, g ^ 1) for g in range(gx)]
    last = bands[:, ny - 1]
    slab = lax.dynamic_index_in_dim(bands, jnp.where(odd == 0, nx - 1, 0), 0, keepdims=False)
    yother = lax.ppermute(last, BOTH, next_core)
    yown = lax.ppermute(last, BOTH, same)
    xhalo = lax.ppermute(slab, BOTH, x_pairs)
    other = lax.ppermute(bands, "gx", partner)
    other_pot = lax.ppermute(pot, "gx", partner)

    gram = half_gram(place, bands, pot)
    gram = half_gram(place, other, other_pot, (gram,))
    sent = add_cross(
        scale, inner, place, gram, bands, other, yown, yother, xhalo, eigenvectors
    )
    groups = [[o * inner + i for i in range(inner)] for o in range(outer)]
    arrived = exchanged(sent, "gyz", groups)
    sent = middle(place, arrived, outer, gx // 2)
    groups = [
        [(2 * c + k) * gyz + o * inner + i for o in range(outer) for c in range(gx // 2)]
        for i in range(inner)
        for k in range(2)
    ]
    arrived = exchanged(sent, BOTH, groups)
    rows, mine = finish(arrived)
    theirs = lax.ppermute(mine, "gx", partner)
    corr, hamil, rotated = rotate(place, bands.reshape(cells, nb), rows, mine, theirs)
    return corr, hamil, rotated.reshape(bands.shape)


def solution(mesh):
    in_specs = (P("gx", "gyz", None, None), P("gx", "gyz", None), P("gyz", None))
    out_specs = (P("gyz", None), P("gyz", None), P("gx", "gyz", None, None))
    return jax.shard_map(
        projected, mesh=mesh, in_specs=in_specs, out_specs=out_specs, check_vma=False
    )
```

```python
import functools

import jax
import jax.numpy as jnp
from jax import lax
from jax.experimental import pallas as pl
from jax.experimental.pallas import tpu as pltpu
from jax.sharding import PartitionSpec as P


F32 = jnp.float32
BF16 = jnp.bfloat16
BOTH = ("gx", "gyz")

VMEM = pl.BlockSpec(memory_space=pltpu.VMEM)
SMEM = pl.BlockSpec(memory_space=pltpu.SMEM)


def over_rows(a, b):
    return lax.dot_general(a, b, (((0,), (0,)), ((), ())), preferred_element_type=F32)


def call(kernel, out_shape, in_specs, args, scratch=(), flops=0):
    many = isinstance(out_shape, tuple)
    moved = sum(a.size * a.dtype.itemsize for a in args)
    return pl.pallas_call(
        kernel,
        out_shape=out_shape,
        in_specs=in_specs,
        out_specs=(VMEM,) * len(out_shape) if many else VMEM,
        scratch_shapes=list(scratch),
        cost_estimate=pl.CostEstimate(flops=flops, bytes_accessed=moved, transcendentals=0),
        compiler_params=pltpu.CompilerParams(vmem_limit_bytes=20 << 20),
    )(*args)


def half_kernel(place_ref, bands_ref, pot_ref, *refs):
    nx, ny, nz, nb = bands_ref.shape
    right_ref, gram_ref = refs[-1], refs[-2]
    row = lax.broadcasted_iota(jnp.int32, (nz, nb), 0)
    half = jnp.where(place_ref[0] == 1, 0.5, 0.0).astype(F32)

    def tiles_at(x):
        return [bands_ref[x, y].astype(F32) for y in range(ny)]

    def slab(x, first):
        pot = jnp.transpose(pot_ref[:, pl.ds(x, 1), :].reshape(ny, nz))
        factor = 0.5 + half * (2.0 + pot)
        tiles = tiles_at(x)
        below = None if first else tiles_at(x - 1)
        for y in range(ny):
            total = jnp.where(row > 0, pltpu.roll(tiles[y], 1, 0), 0.0)
            if y > 0:
                total += tiles[y - 1]
            if not first:
                total += below[y]
            right_ref[x, y] = (factor[:, y : y + 1] * tiles[y] - half * total).astype(BF16)

    def step(x, carry):
        slab(x, False)
        return carry

    slab(0, True)
    lax.fori_loop(1, nx, step, 0)
    gram = over_rows(bands_ref[...].reshape(-1, nb), right_ref[...].reshape(-1, nb))
    if len(refs) > 2:
        gram += refs[0][...]
    gram_ref[...] = gram


def half_gram(place, bands, pot, given=()):
    nb = bands.shape[-1]
    return call(
        half_kernel,
        jax.ShapeDtypeStruct((nb, nb), F32),
        [SMEM] + [VMEM] * (2 + len(given)),
        (place, bands, pot, *given),
        scratch=[pltpu.VMEM(bands.shape, BF16)],
        flops=2 * bands.size * nb,
    )


def cross_kernel(
    scale, place_ref, gram_ref, own_ref, other_ref, yown_ref, yother_ref, xhalo_ref, out_ref
):
    _, _, nb = xhalo_ref.shape
    nx = yown_ref.shape[0]

    def rows(value):
        return value.reshape(-1, nb)

    cross = over_rows(rows(own_ref[:, 0]), rows(yown_ref[...]))
    cross += over_rows(rows(other_ref[:, 0]), rows(yother_ref[...]))
    slab = jnp.where(place_ref[1] == 0, other_ref[0], own_ref[nx - 1])
    cross += over_rows(rows(slab), rows(xhalo_ref[...]))
    inside = over_rows(rows(own_ref[0]), rows(other_ref[nx - 1]))
    gram = gram_ref[...] - 0.5 * (cross + jnp.where(place_ref[0] == 1, inside, 0.0))
    out_ref[...] = (scale * (gram + jnp.transpose(gram))).astype(BF16)


def add_cross(scale, place, gram, own, other, yown, yother, xhalo):
    nb = gram.shape[0]
    halo_rows = (yown.size + yother.size + xhalo.size) // nb
    return call(
        functools.partial(cross_kernel, scale),
        jax.ShapeDtypeStruct((nb, nb), BF16),
        [SMEM] + [VMEM] * 6,
        (place, gram, own, other, yown, yother, xhalo),
        flops=2 * halo_rows * nb * nb,
    )


def finish_kernel(in_ref, rows_ref):
    total = in_ref[0].astype(F32)
    for s in range(1, in_ref.shape[0]):
        total += in_ref[s].astype(F32)
    for c in range(rows_ref.shape[0]):
        rows_ref[c] = total


def finish(arrived, copies):
    _, depth, nb = arrived.shape
    return call(finish_kernel, jax.ShapeDtypeStruct((copies, depth, nb), F32), [VMEM], (arrived,))


def rotate_kernel(place_ref, bands_ref, mine_ref, theirs_ref, out_ref):
    core = place_ref[0]
    width = mine_ref.shape[1]
    block = out_ref.shape[0]
    mine, theirs = mine_ref[...], theirs_ref[...]
    start = pl.multiple_of(pl.program_id(0) * block, block)
    some = bands_ref[pl.ds(start, block)]
    left = jnp.where(core == 0, mine, theirs)
    right = jnp.where(core == 0, theirs, mine)
    out_ref[:, :width] = jnp.dot(some, left, preferred_element_type=F32).astype(BF16)
    out_ref[:, width:] = jnp.dot(some, right, preferred_element_type=F32).astype(BF16)


def rotate(place, flat, mine, theirs):
    cells, nb = flat.shape
    steps = 5
    block = cells // steps
    return pl.pallas_call(
        rotate_kernel,
        grid=(steps,),
        out_shape=jax.ShapeDtypeStruct((cells, nb), BF16),
        in_specs=[SMEM] + [VMEM] * 3,
        out_specs=pl.BlockSpec((block, nb), lambda i: (i, 0)),
        cost_estimate=pl.CostEstimate(
            flops=2 * cells * nb * nb, bytes_accessed=4 * cells * nb, transcendentals=0
        ),
        compiler_params=pltpu.CompilerParams(vmem_limit_bytes=20 << 20),
        name="rotate",
    )(place, flat, mine, theirs)


def pairs_of(gx, gyz):
    def at(g, r):
        return g * gyz + r

    same, next_core, x = [], [], []
    for chip in range(gx // 2):
        for r in range(gyz - 1):
            same.append((at(2 * chip + 1, r), at(2 * chip + 1, r + 1)))
            next_core.append((at(2 * chip, r), at(2 * chip + 1, r + 1)))
    for chip in range(gx // 2 - 1):
        for r in range(gyz):
            if r % 2 == 0:
                x.append((at(2 * chip + 1, r), at(2 * chip + 3, r)))
            else:
                x.append((at(2 * chip + 2, r), at(2 * chip + 1, r)))
    return same, next_core, x


def exchanged(x, axis):
    return lax.all_to_all(x, axis, 0, 0, tiled=True)


def projected(bands, potential, eigenvectors):
    nx, ny, nz, nb = bands.shape
    gx, gyz = lax.axis_size("gx"), lax.axis_size("gyz")
    depth = eigenvectors.shape[0]
    core = lax.rem(lax.axis_index("gx"), 2)
    odd = lax.rem(lax.axis_index("gyz"), 2)
    cells = nx * ny * nz
    scale = 1.0 / (cells * gyz)
    place = jnp.stack((core, odd)).astype(jnp.int32)
    pot = jnp.transpose(potential, (1, 0, 2))

    half = lax.dynamic_slice_in_dim(eigenvectors, core * (nb // 2), nb // 2, axis=1)
    mine = exchanged(jnp.broadcast_to(half[None], (gyz, *half.shape)), "gyz")
    mine = mine.reshape(nb, nb // 2)

    same, next_core, x_pairs = pairs_of(gx, gyz)
    partner = [(g, g ^ 1) for g in range(gx)]
    last = bands[:, ny - 1]
    slab = lax.dynamic_index_in_dim(bands, jnp.where(odd == 0, nx - 1, 0), 0, keepdims=False)
    yother = lax.ppermute(last, BOTH, next_core)
    yown = lax.ppermute(last, BOTH, same)
    xhalo = lax.ppermute(slab, BOTH, x_pairs)
    other = lax.ppermute(bands, "gx", partner)
    other_pot = lax.ppermute(pot, "gx", partner)

    gram = half_gram(place, bands, pot)
    gram = half_gram(place, other, other_pot, (gram,))
    gram = add_cross(scale, place, gram, bands, other, yown, yother, xhalo)
    arrived = exchanged(gram.reshape(gyz, depth, nb), "gyz")
    rows = finish(arrived, gx)
    parts = exchanged(rows, "gx")
    sums = parts.reshape(gx // 2, 2, depth, nb).sum(axis=0)
    theirs = lax.ppermute(mine, "gx", partner)
    rotated = rotate(place, bands.reshape(cells, nb), mine, theirs)
    return sums[0], sums[1], rotated.reshape(bands.shape)


def solution(mesh):
    in_specs = (P("gx", "gyz", None, None), P("gx", "gyz", None), P("gyz", None))
    out_specs = (P("gyz", None), P("gyz", None), P("gx", "gyz", None, None))
    return jax.shard_map(
        projected, mesh=mesh, in_specs=in_specs, out_specs=out_specs, check_vma=False
    )
```

```python
import functools

import jax
import jax.numpy as jnp
from jax import lax
from jax.experimental import pallas as pl
from jax.experimental.pallas import tpu as pltpu
from jax.sharding import PartitionSpec as P


F32 = jnp.float32
BF16 = jnp.bfloat16
BOTH = ("gx", "gyz")

VMEM = pl.BlockSpec(memory_space=pltpu.VMEM)
SMEM = pl.BlockSpec(memory_space=pltpu.SMEM)


def over_rows(a, b):
    return lax.dot_general(a, b, (((0,), (0,)), ((), ())), preferred_element_type=F32)


def call(kernel, out_shape, in_specs, args, scratch=(), flops=0):
    many = isinstance(out_shape, tuple)
    moved = sum(a.size * a.dtype.itemsize for a in args)
    return pl.pallas_call(
        kernel,
        out_shape=out_shape,
        in_specs=in_specs,
        out_specs=(VMEM,) * len(out_shape) if many else VMEM,
        scratch_shapes=list(scratch),
        cost_estimate=pl.CostEstimate(flops=flops, bytes_accessed=moved, transcendentals=0),
        compiler_params=pltpu.CompilerParams(vmem_limit_bytes=10 << 20),
    )(*args)


def half_kernel(place_ref, bands_ref, pot_ref, *refs):
    nx, ny, nz, nb = bands_ref.shape
    right_ref = refs[-1]
    given = refs[0][...] if refs[1].shape == (nb, nb) else None
    gram_ref = refs[1] if given is not None else refs[0]
    if given is None:
        refs[1][...] = bands_ref[jnp.where(place_ref[1] == 0, nx - 1, 0)]
    row = lax.broadcasted_iota(jnp.int32, (nz, nb), 0)
    half = jnp.where(place_ref[0] == 1, 0.5, 0.0).astype(F32)

    def tiles_at(x):
        return [bands_ref[x, y].astype(F32) for y in range(ny)]

    def slab(x, first):
        pot = jnp.transpose(pot_ref[:, pl.ds(x, 1), :].reshape(ny, nz))
        factor = 0.5 + half * (2.0 + pot)
        tiles = tiles_at(x)
        below = None if first else tiles_at(x - 1)
        for y in range(ny):
            total = jnp.where(row > 0, pltpu.roll(tiles[y], 1, 0), 0.0)
            if y > 0:
                total += tiles[y - 1]
            if not first:
                total += below[y]
            right_ref[x, y] = (factor[:, y : y + 1] * tiles[y] - half * total).astype(BF16)

    def step(x, carry):
        slab(x, False)
        return carry

    slab(0, True)
    lax.fori_loop(1, nx, step, 0, unroll=True)
    gram = over_rows(bands_ref[...].reshape(-1, nb), right_ref[...].reshape(-1, nb))
    gram_ref[...] = gram if given is None else given + gram


def half_gram(place, bands, pot, given=()):
    nb = bands.shape[-1]
    gram = jax.ShapeDtypeStruct((nb, nb), F32)
    return call(
        half_kernel,
        gram if given else (gram, jax.ShapeDtypeStruct(bands.shape[1:], BF16)),
        [SMEM] + [VMEM] * (2 + len(given)),
        (place, bands, pot, *given),
        scratch=[pltpu.VMEM(bands.shape, BF16)],
        flops=2 * bands.size * nb,
    )


def cross_kernel(
    scale, place_ref, gram_ref, own_ref, other_ref, yown_ref, yother_ref, xhalo_ref, coef_ref, out_ref
):
    _, _, nb = xhalo_ref.shape
    nx = yown_ref.shape[0]
    groups, depth = out_ref.shape[0], coef_ref.shape[0]

    def rows(value):
        return value.reshape(-1, nb)

    cross = over_rows(rows(own_ref[:, 0]), rows(yown_ref[...]))
    cross += over_rows(rows(other_ref[:, 0]), rows(yother_ref[...]))
    slab = jnp.where(place_ref[1] == 0, other_ref[0], own_ref[nx - 1])
    cross += over_rows(rows(slab), rows(xhalo_ref[...]))
    inside = over_rows(rows(own_ref[0]), rows(other_ref[nx - 1]))
    gram = gram_ref[...] - 0.5 * (cross + jnp.where(place_ref[0] == 1, inside, 0.0))
    total = (scale * (gram + jnp.transpose(gram))).astype(BF16)
    total = total.reshape(nb // (groups * depth), groups, depth, nb)
    for d in range(groups):
        out_ref[d, 0 : nb // groups] = rows(total[:, d])
        out_ref[d, nb // groups :] = coef_ref[...]


def add_cross(scale, groups, place, gram, own, other, yown, yother, xhalo, coef):
    nb = gram.shape[0]
    depth = coef.shape[0]
    halo_rows = (yown.size + yother.size + xhalo.size) // nb
    return call(
        functools.partial(cross_kernel, scale),
        jax.ShapeDtypeStruct((groups, nb // groups + depth, nb), BF16),
        [SMEM] + [VMEM] * 7,
        (place, gram, own, other, yown, yother, xhalo, coef),
        flops=2 * halo_rows * nb * nb,
    )


def middle_kernel(place_ref, in_ref, out_ref):
    sources, height, nb = in_ref.shape
    targets, _, _ = out_ref.shape
    depth = (height * targets - nb * targets // sources) // targets
    width = nb // 2
    total = in_ref[0, 0 : height - depth].astype(F32)
    for s in range(1, sources):
        total += in_ref[s, 0 : height - depth].astype(F32)
    total = total.astype(BF16).reshape(targets, depth, nb)
    upper = sources // 2
    for s in range(sources):
        coef = in_ref[s, height - depth :]
        coef = jnp.where(place_ref[0] == 0, coef[:, :width], coef[:, width:])
        first = depth + (s % upper) * depth
        lane = (s // upper) * width
        for t in range(targets):
            out_ref[t, first : first + depth, lane : lane + width] = coef
    for t in range(targets):
        out_ref[t, 0:depth] = total[t]


def middle(place, arrived, targets):
    sources, height, nb = arrived.shape
    depth = height - nb // sources
    return call(
        middle_kernel,
        jax.ShapeDtypeStruct((targets, depth + sources * depth // 2, nb), BF16),
        [SMEM, VMEM],
        (place, arrived),
    )


def last_kernel(in_ref, rows_ref, coef_ref):
    sources, height, nb = in_ref.shape
    copies, depth, _ = rows_ref.shape
    total = in_ref[0, 0:depth].astype(F32)
    for s in range(1, sources):
        total += in_ref[s, 0:depth].astype(F32)
    for c in range(copies):
        rows_ref[c] = total
    plane = 2 * (height - depth)
    for s in range(sources):
        for part in range(2):
            start = s * plane + part * (plane // 2)
            coef_ref[start : start + plane // 2] = in_ref[
                s, depth:, part * (nb // 2) : (part + 1) * (nb // 2)
            ]


def finish(arrived, copies, depth):
    _, _, nb = arrived.shape
    return call(
        last_kernel,
        (
            jax.ShapeDtypeStruct((copies, depth, nb), F32),
            jax.ShapeDtypeStruct((nb, nb // 2), BF16),
        ),
        [VMEM],
        (arrived,),
    )


def pairs_of(gx, gyz):
    def at(g, r):
        return g * gyz + r

    same, next_core, x = [], [], []
    for chip in range(gx // 2):
        for r in range(gyz - 1):
            same.append((at(2 * chip + 1, r), at(2 * chip + 1, r + 1)))
            next_core.append((at(2 * chip, r), at(2 * chip + 1, r + 1)))
    for chip in range(gx // 2 - 1):
        for r in range(gyz):
            if r % 2 == 0:
                x.append((at(2 * chip + 1, r), at(2 * chip + 3, r)))
            else:
                x.append((at(2 * chip + 2, r), at(2 * chip + 1, r)))
    return same, next_core, x


def exchanged(x, axis, groups=None):
    return lax.all_to_all(x, axis, 0, 0, tiled=True, axis_index_groups=groups)


def projected(bands, potential, eigenvectors):
    nx, ny, nz, nb = bands.shape
    gx, gyz = lax.axis_size("gx"), lax.axis_size("gyz")
    depth = eigenvectors.shape[0]
    inner = 8
    outer = gyz // inner
    core = lax.rem(lax.axis_index("gx"), 2)
    odd = lax.rem(lax.axis_index("gyz"), 2)
    cells = nx * ny * nz
    scale = 1.0 / (cells * gyz)
    place = jnp.stack((core, odd)).astype(jnp.int32)
    pot = jnp.transpose(potential, (1, 0, 2))

    same, next_core, x_pairs = pairs_of(gx, gyz)
    partner = [(g, g ^ 1) for g in range(gx)]
    last = bands[:, ny - 1]
    yother = lax.ppermute(last, BOTH, next_core)
    yown = lax.ppermute(last, BOTH, same)
    other = lax.ppermute(bands, "gx", partner)
    other_pot = lax.ppermute(pot, "gx", partner)
    gram, slab = half_gram(place, bands, pot)
    xhalo = lax.ppermute(slab, BOTH, x_pairs)
    gram = half_gram(place, other, other_pot, (gram,))
    sent = add_cross(
        scale, inner, place, gram, bands, other, yown, yother, xhalo, eigenvectors
    )
    arrived = exchanged(sent, "gyz", [[o * inner + i for i in range(inner)] for o in range(outer)])
    sent = middle(place, arrived, outer)
    arrived = exchanged(sent, "gyz", [[o * inner + i for o in range(outer)] for i in range(inner)])
    rows, coef = finish(arrived, gx, depth)
    coef_other = lax.ppermute(coef, "gx", partner)
    parts = exchanged(rows, "gx")
    sums = parts.reshape(gx // 2, 2, *parts.shape[1:]).sum(axis=0)

    left = jnp.where(core == 0, coef, coef_other)
    right = jnp.where(core == 0, coef_other, coef)
    rotated = jnp.dot(
        bands.reshape(cells, nb),
        jnp.concatenate((left, right), axis=1),
        preferred_element_type=F32,
    ).astype(BF16)
    return sums[0], sums[1], rotated.reshape(bands.shape)


def solution(mesh):
    in_specs = (P("gx", "gyz", None, None), P("gx", "gyz", None), P("gyz", None))
    out_specs = (P("gyz", None), P("gyz", None), P("gx", "gyz", None, None))
    return jax.shard_map(
        projected, mesh=mesh, in_specs=in_specs, out_specs=out_specs, check_vma=False
    )
```

```python
import functools

import jax
import jax.numpy as jnp
from jax import lax
from jax.experimental import pallas as pl
from jax.experimental.pallas import tpu as pltpu
from jax.sharding import PartitionSpec as P


F32 = jnp.float32
BF16 = jnp.bfloat16
BOTH = ("gx", "gyz")

PIECES = 3

VMEM = pl.BlockSpec(memory_space=pltpu.VMEM)
HBM = pl.BlockSpec(memory_space=pltpu.HBM)
SMEM = pl.BlockSpec(memory_space=pltpu.SMEM)


def over_rows(a, b):
    return lax.dot_general(a, b, (((0,), (0,)), ((), ())), preferred_element_type=F32)


def call(kernel, out_shape, in_specs, args, scratch=(), flops=0):
    many = isinstance(out_shape, tuple)
    moved = sum(a.size * a.dtype.itemsize for a in args)
    return pl.pallas_call(
        kernel,
        out_shape=out_shape,
        in_specs=in_specs,
        out_specs=(VMEM,) * len(out_shape) if many else VMEM,
        scratch_shapes=list(scratch),
        cost_estimate=pl.CostEstimate(flops=flops, bytes_accessed=moved, transcendentals=0),
        compiler_params=pltpu.CompilerParams(vmem_limit_bytes=10 << 20),
    )(*args)


def prepare_kernel(place_ref, bands_ref, pot_ref, held_ref, last_ref, slab_ref, pot_vmem, sems):
    nx, ny, nz, _ = bands_ref.shape
    sent = jnp.where(place_ref[1] == 0, nx - 1, 0)
    copies = (
        pltpu.make_async_copy(pot_ref, pot_vmem, sems.at[0]),
        pltpu.make_async_copy(bands_ref.at[:, ny - 1], last_ref, sems.at[1]),
        pltpu.make_async_copy(bands_ref.at[sent], slab_ref, sems.at[2]),
        pltpu.make_async_copy(bands_ref, held_ref.at[pl.ds(0, nx)], sems.at[3]),
    )
    for copy in copies:
        copy.start()
    copies[0].wait()
    rest = pot_vmem[...].reshape(nx * ny, nz)
    for piece in range(PIECES):
        part = rest.astype(BF16)
        held_ref[nx, piece, 0 : nx * ny, 0:nz] = part
        rest = rest - part.astype(F32)
    for copy in copies[1:]:
        copy.wait()


def prepare(place, bands, pot):
    nx, ny, nz, nb = bands.shape
    assert ny >= PIECES and nx * ny <= nz <= nb
    shapes = ((nx + 1, ny, nz, nb), (nx, nz, nb), (ny, nz, nb))
    bands, pot = (pltpu.with_memory_space_constraint(x, pltpu.HBM) for x in (bands, pot))
    return call(
        prepare_kernel,
        tuple(jax.ShapeDtypeStruct(s, BF16) for s in shapes),
        [SMEM, HBM, HBM],
        (place, bands, pot),
        scratch=[pltpu.VMEM(pot.shape, F32), pltpu.SemaphoreType.DMA((4,))],
    )


def half_kernel(place_ref, held_ref, *refs):
    gram_ref, right_ref, pot_ref = refs[-3:]
    nx, ny, nz, nb = right_ref.shape
    row = lax.broadcasted_iota(jnp.int32, (nz, nb), 0)
    half = jnp.where(place_ref[0] == 1, 0.5, 0.0).astype(F32)
    pieces = [held_ref[nx, p, 0 : nx * ny, 0:nz].astype(F32) for p in range(PIECES)]
    pot_ref[...] = ((pieces[2] + pieces[1]) + pieces[0]).reshape(ny, nx, nz)

    def tiles_at(x):
        return [held_ref[x, y].astype(F32) for y in range(ny)]

    def slab(x, first):
        pot = jnp.transpose(pot_ref[:, pl.ds(x, 1), :].reshape(ny, nz))
        factor = 0.5 + half * (2.0 + pot)
        tiles = tiles_at(x)
        below = None if first else tiles_at(x - 1)
        for y in range(ny):
            total = jnp.where(row > 0, pltpu.roll(tiles[y], 1, 0), 0.0)
            if y > 0:
                total += tiles[y - 1]
            if not first:
                total += below[y]
            right_ref[x, y] = (factor[:, y : y + 1] * tiles[y] - half * total).astype(BF16)

    def step(x, carry):
        slab(x, False)
        return carry

    slab(0, True)
    lax.fori_loop(1, nx, step, 0, unroll=True)
    gram = over_rows(held_ref[0:nx].reshape(-1, nb), right_ref[...].reshape(-1, nb))
    gram_ref[...] = refs[0][...] + gram if len(refs) > 3 else gram


def half_gram(place, held, given=()):
    nx, ny, nz, nb = held.shape
    nx -= 1
    return call(
        half_kernel,
        jax.ShapeDtypeStruct((nb, nb), F32),
        [SMEM] + [VMEM] * (1 + len(given)),
        (place, held, *given),
        scratch=[pltpu.VMEM((nx, ny, nz, nb), BF16), pltpu.VMEM((ny, nx, nz), F32)],
        flops=2 * nx * ny * nz * nb * nb,
    )


def cross_kernel(
    scale, place_ref, gram_ref, own_ref, other_ref, yown_ref, yother_ref, xhalo_ref, coef_ref, out_ref
):
    _, _, nb = xhalo_ref.shape
    nx = yown_ref.shape[0]
    groups, depth = out_ref.shape[0], coef_ref.shape[0]

    def rows(value):
        return value.reshape(-1, nb)

    cross = over_rows(rows(own_ref[0:nx, 0]), rows(yown_ref[...]))
    cross += over_rows(rows(other_ref[0:nx, 0]), rows(yother_ref[...]))
    slab = jnp.where(place_ref[1] == 0, other_ref[0], own_ref[nx - 1])
    cross += over_rows(rows(slab), rows(xhalo_ref[...]))
    inside = over_rows(rows(own_ref[0]), rows(other_ref[nx - 1]))
    gram = gram_ref[...] - 0.5 * (cross + jnp.where(place_ref[0] == 1, inside, 0.0))
    total = (scale * (gram + jnp.transpose(gram))).astype(BF16)
    total = total.reshape(nb // (groups * depth), groups, depth, nb)
    for d in range(groups):
        out_ref[d, 0 : nb // groups] = rows(total[:, d])
        out_ref[d, nb // groups :] = coef_ref[...]


def add_cross(scale, groups, place, gram, own, other, yown, yother, xhalo, coef):
    nb = gram.shape[0]
    depth = coef.shape[0]
    halo_rows = (yown.size + yother.size + xhalo.size) // nb
    return call(
        functools.partial(cross_kernel, scale),
        jax.ShapeDtypeStruct((groups, nb // groups + depth, nb), BF16),
        [SMEM] + [VMEM] * 7,
        (place, gram, own, other, yown, yother, xhalo, coef),
        flops=2 * halo_rows * nb * nb,
    )


def middle_kernel(place_ref, in_ref, out_ref):
    sources, height, nb = in_ref.shape
    targets, _, _ = out_ref.shape
    depth = (height * targets - nb * targets // sources) // targets
    width = nb // 2
    total = in_ref[0, 0 : height - depth].astype(F32)
    for s in range(1, sources):
        total += in_ref[s, 0 : height - depth].astype(F32)
    total = total.astype(BF16).reshape(targets, depth, nb)
    upper = sources // 2
    for s in range(sources):
        coef = in_ref[s, height - depth :]
        coef = jnp.where(place_ref[0] == 0, coef[:, :width], coef[:, width:])
        first = depth + (s % upper) * depth
        lane = (s // upper) * width
        for t in range(targets):
            out_ref[t, first : first + depth, lane : lane + width] = coef
    for t in range(targets):
        out_ref[t, 0:depth] = total[t]


def middle(place, arrived, targets):
    sources, height, nb = arrived.shape
    depth = height - nb // sources
    return call(
        middle_kernel,
        jax.ShapeDtypeStruct((targets, depth + sources * depth // 2, nb), BF16),
        [SMEM, VMEM],
        (place, arrived),
    )


def last_kernel(in_ref, rows_ref, coef_ref):
    sources, height, nb = in_ref.shape
    copies, depth, _ = rows_ref.shape
    total = in_ref[0, 0:depth].astype(F32)
    for s in range(1, sources):
        total += in_ref[s, 0:depth].astype(F32)
    for c in range(copies):
        rows_ref[c] = total
    plane = 2 * (height - depth)
    for s in range(sources):
        for part in range(2):
            start = s * plane + part * (plane // 2)
            coef_ref[start : start + plane // 2] = in_ref[
                s, depth:, part * (nb // 2) : (part + 1) * (nb // 2)
            ]


def finish(arrived, copies, depth):
    _, _, nb = arrived.shape
    return call(
        last_kernel,
        (
            jax.ShapeDtypeStruct((copies, depth, nb), F32),
            jax.ShapeDtypeStruct((nb, nb // 2), BF16),
        ),
        [VMEM],
        (arrived,),
    )


def pairs_of(gx, gyz):
    def at(g, r):
        return g * gyz + r

    same, next_core, x = [], [], []
    for chip in range(gx // 2):
        for r in range(gyz - 1):
            same.append((at(2 * chip + 1, r), at(2 * chip + 1, r + 1)))
            next_core.append((at(2 * chip, r), at(2 * chip + 1, r + 1)))
    for chip in range(gx // 2 - 1):
        for r in range(gyz):
            if r % 2 == 0:
                x.append((at(2 * chip + 1, r), at(2 * chip + 3, r)))
            else:
                x.append((at(2 * chip + 2, r), at(2 * chip + 1, r)))
    return same, next_core, x


def exchanged(x, axis, groups=None):
    return lax.all_to_all(x, axis, 0, 0, tiled=True, axis_index_groups=groups)


def projected(bands, potential, eigenvectors):
    nx, ny, nz, nb = bands.shape
    gx, gyz = lax.axis_size("gx"), lax.axis_size("gyz")
    depth = eigenvectors.shape[0]
    inner = 8
    outer = gyz // inner
    core = lax.rem(lax.axis_index("gx"), 2)
    odd = lax.rem(lax.axis_index("gyz"), 2)
    cells = nx * ny * nz
    scale = 1.0 / (cells * gyz)
    place = jnp.stack((core, odd)).astype(jnp.int32)
    pot = jnp.transpose(potential, (1, 0, 2))

    own, last, slab = prepare(place, bands, pot)
    same, next_core, x_pairs = pairs_of(gx, gyz)
    partner = [(g, g ^ 1) for g in range(gx)]
    yother = lax.ppermute(last, BOTH, next_core)
    yown = lax.ppermute(last, BOTH, same)
    other = lax.ppermute(own, "gx", partner)
    xhalo = lax.ppermute(slab, BOTH, x_pairs)
    gram = half_gram(place, own)
    gram = half_gram(place, other, (gram,))
    sent = add_cross(
        scale, inner, place, gram, own, other, yown, yother, xhalo, eigenvectors
    )
    arrived = exchanged(sent, "gyz", [[o * inner + i for i in range(inner)] for o in range(outer)])
    sent = middle(place, arrived, outer)
    arrived = exchanged(sent, "gyz", [[o * inner + i for o in range(outer)] for i in range(inner)])
    rows, coef = finish(arrived, gx, depth)
    coef_other = lax.ppermute(coef, "gx", partner)
    parts = exchanged(rows, "gx")
    sums = parts.reshape(gx // 2, 2, *parts.shape[1:]).sum(axis=0)

    left = jnp.where(core == 0, coef, coef_other)
    right = jnp.where(core == 0, coef_other, coef)
    rotated = jnp.dot(
        bands.reshape(cells, nb),
        jnp.concatenate((left, right), axis=1),
        preferred_element_type=F32,
    ).astype(BF16)
    return sums[0], sums[1], rotated.reshape(bands.shape)


def solution(mesh):
    in_specs = (P("gx", "gyz", None, None), P("gx", "gyz", None), P("gyz", None))
    out_specs = (P("gyz", None), P("gyz", None), P("gx", "gyz", None, None))
    return jax.shard_map(
        projected, mesh=mesh, in_specs=in_specs, out_specs=out_specs, check_vma=False
    )
```

```python
import functools

import jax
import jax.numpy as jnp
from jax import lax
from jax.experimental import pallas as pl
from jax.experimental.pallas import tpu as pltpu
from jax.sharding import PartitionSpec as P


F32 = jnp.float32
BF16 = jnp.bfloat16
BOTH = ("gx", "gyz")

PIECES = 3

VMEM = pl.BlockSpec(memory_space=pltpu.VMEM)
HBM = pl.BlockSpec(memory_space=pltpu.HBM)
SMEM = pl.BlockSpec(memory_space=pltpu.SMEM)


def over_rows(a, b):
    return lax.dot_general(a, b, (((0,), (0,)), ((), ())), preferred_element_type=F32)


def call(kernel, out_shape, in_specs, args, scratch=(), flops=0):
    many = isinstance(out_shape, tuple)
    moved = sum(a.size * a.dtype.itemsize for a in args)
    return pl.pallas_call(
        kernel,
        out_shape=out_shape,
        in_specs=in_specs,
        out_specs=(VMEM,) * len(out_shape) if many else VMEM,
        scratch_shapes=list(scratch),
        cost_estimate=pl.CostEstimate(flops=flops, bytes_accessed=moved, transcendentals=0),
        compiler_params=pltpu.CompilerParams(vmem_limit_bytes=10 << 20),
    )(*args)


def prepare_kernel(place_ref, bands_ref, pot_ref, held_ref, last_ref, slab_ref, pot_vmem, sems):
    nx, ny, nz, _ = bands_ref.shape
    sent = jnp.where(place_ref[1] == 0, nx - 1, 0)
    copies = (
        pltpu.make_async_copy(pot_ref, pot_vmem, sems.at[0]),
        pltpu.make_async_copy(bands_ref.at[:, ny - 1], last_ref, sems.at[1]),
        pltpu.make_async_copy(bands_ref.at[sent], slab_ref, sems.at[2]),
        pltpu.make_async_copy(bands_ref, held_ref.at[pl.ds(0, nx)], sems.at[3]),
    )
    for copy in copies:
        copy.start()
    copies[0].wait()
    rest = pot_vmem[...].reshape(nx * ny, nz)
    for piece in range(PIECES):
        part = rest.astype(BF16)
        held_ref[nx, piece, 0 : nx * ny, 0:nz] = part
        rest = rest - part.astype(F32)
    for copy in copies[1:]:
        copy.wait()


def prepare(place, bands, pot):
    nx, ny, nz, nb = bands.shape
    assert ny >= PIECES and nx * ny <= nz <= nb
    shapes = ((nx + 1, ny, nz, nb), (nx, nz, nb), (ny, nz, nb))
    bands, pot = (pltpu.with_memory_space_constraint(x, pltpu.HBM) for x in (bands, pot))
    return call(
        prepare_kernel,
        tuple(jax.ShapeDtypeStruct(s, BF16) for s in shapes),
        [SMEM, HBM, HBM],
        (place, bands, pot),
        scratch=[pltpu.VMEM(pot.shape, F32), pltpu.SemaphoreType.DMA((4,))],
    )


def half_kernel(place_ref, held_ref, *refs):
    gram_ref, right_ref, pot_ref = refs[-3:]
    nx, ny, nz, nb = right_ref.shape
    row = lax.broadcasted_iota(jnp.int32, (nz, nb), 0)

    def tiles_at(x):
        return [held_ref[x, y].astype(F32) for y in range(ny)]

    def slab(x):
        pot = jnp.transpose(pot_ref[:, pl.ds(x, 1), :].reshape(ny, nz))
        factor = 1.5 + 0.5 * pot
        tiles = tiles_at(x)
        below = None if x == 0 else tiles_at(x - 1)
        for y in range(ny):
            total = jnp.where(row > 0, pltpu.roll(tiles[y], 1, 0), 0.0)
            if y > 0:
                total += tiles[y - 1]
            if x > 0:
                total += below[y]
            right_ref[x, y] = (factor[:, y : y + 1] * tiles[y] - 0.5 * total).astype(BF16)

    def store(gram):
        gram_ref[...] = refs[0][...] + gram if len(refs) > 3 else gram

    bands = held_ref[0:nx].reshape(-1, nb)

    @pl.when(place_ref[0] == 1)
    def _():
        pieces = [held_ref[nx, p, 0 : nx * ny, 0:nz].astype(F32) for p in range(PIECES)]
        pot_ref[...] = ((pieces[2] + pieces[1]) + pieces[0]).reshape(ny, nx, nz)
        for x in range(nx):
            slab(x)
        store(over_rows(bands, right_ref[...].reshape(-1, nb)))

    @pl.when(place_ref[0] == 0)
    def _():
        store(over_rows(bands, bands))


def half_gram(place, held, given=()):
    nx, ny, nz, nb = held.shape
    nx -= 1
    return call(
        half_kernel,
        jax.ShapeDtypeStruct((nb, nb), F32),
        [SMEM] + [VMEM] * (1 + len(given)),
        (place, held, *given),
        scratch=[pltpu.VMEM((nx, ny, nz, nb), BF16), pltpu.VMEM((ny, nx, nz), F32)],
        flops=2 * nx * ny * nz * nb * nb,
    )


def cross_kernel(
    scale, place_ref, gram_ref, own_ref, other_ref, yown_ref, yother_ref, xhalo_ref, coef_ref, out_ref
):
    _, _, nb = xhalo_ref.shape
    nx = yown_ref.shape[0]
    groups, depth = out_ref.shape[0], coef_ref.shape[0]

    def rows(value):
        return value.reshape(-1, nb)

    def send(total):
        total = total.astype(BF16).reshape(nb // (groups * depth), groups, depth, nb)
        for d in range(groups):
            out_ref[d, 0 : nb // groups] = rows(total[:, d])
            out_ref[d, nb // groups :] = coef_ref[...]

    @pl.when(place_ref[0] == 1)
    def _():
        cross = over_rows(rows(own_ref[0:nx, 0]), rows(yown_ref[...]))
        cross += over_rows(rows(other_ref[0:nx, 0]), rows(yother_ref[...]))
        slab = jnp.where(place_ref[1] == 0, other_ref[0], own_ref[nx - 1])
        cross += over_rows(rows(slab), rows(xhalo_ref[...]))
        cross += over_rows(rows(own_ref[0]), rows(other_ref[nx - 1]))
        gram = gram_ref[...] - 0.5 * cross
        send(scale * (gram + jnp.transpose(gram)))

    @pl.when(place_ref[0] == 0)
    def _():
        send(scale * gram_ref[...])


def add_cross(scale, groups, place, gram, own, other, yown, yother, xhalo, coef):
    nb = gram.shape[0]
    depth = coef.shape[0]
    halo_rows = (yown.size + yother.size + xhalo.size) // nb
    return call(
        functools.partial(cross_kernel, scale),
        jax.ShapeDtypeStruct((groups, nb // groups + depth, nb), BF16),
        [SMEM] + [VMEM] * 7,
        (place, gram, own, other, yown, yother, xhalo, coef),
        flops=2 * halo_rows * nb * nb,
    )


def middle_kernel(place_ref, in_ref, out_ref):
    sources, height, nb = in_ref.shape
    targets, _, _ = out_ref.shape
    depth = (height * targets - nb * targets // sources) // targets
    width = nb // 2
    total = in_ref[0, 0 : height - depth].astype(F32)
    for s in range(1, sources):
        total += in_ref[s, 0 : height - depth].astype(F32)
    total = total.astype(BF16).reshape(targets, depth, nb)
    upper = sources // 2
    for s in range(sources):
        coef = in_ref[s, height - depth :]
        coef = jnp.where(place_ref[0] == 0, coef[:, :width], coef[:, width:])
        first = depth + (s % upper) * depth
        lane = (s // upper) * width
        for t in range(targets):
            out_ref[t, first : first + depth, lane : lane + width] = coef
    for t in range(targets):
        out_ref[t, 0:depth] = total[t]


def middle(place, arrived, targets):
    sources, height, nb = arrived.shape
    depth = height - nb // sources
    return call(
        middle_kernel,
        jax.ShapeDtypeStruct((targets, depth + sources * depth // 2, nb), BF16),
        [SMEM, VMEM],
        (place, arrived),
    )


def last_kernel(in_ref, rows_ref, coef_ref):
    sources, height, nb = in_ref.shape
    copies, depth, _ = rows_ref.shape
    total = in_ref[0, 0:depth].astype(F32)
    for s in range(1, sources):
        total += in_ref[s, 0:depth].astype(F32)
    for c in range(copies):
        rows_ref[c] = total
    plane = 2 * (height - depth)
    for s in range(sources):
        for part in range(2):
            start = s * plane + part * (plane // 2)
            coef_ref[start : start + plane // 2] = in_ref[
                s, depth:, part * (nb // 2) : (part + 1) * (nb // 2)
            ]


def finish(arrived, copies, depth):
    _, _, nb = arrived.shape
    return call(
        last_kernel,
        (
            jax.ShapeDtypeStruct((copies, depth, nb), F32),
            jax.ShapeDtypeStruct((nb, nb // 2), BF16),
        ),
        [VMEM],
        (arrived,),
    )


def pairs_of(gx, gyz):
    def at(g, r):
        return g * gyz + r

    same, next_core, x = [], [], []
    for chip in range(gx // 2):
        for r in range(gyz - 1):
            same.append((at(2 * chip + 1, r), at(2 * chip + 1, r + 1)))
            next_core.append((at(2 * chip, r), at(2 * chip + 1, r + 1)))
    for chip in range(gx // 2 - 1):
        for r in range(gyz):
            if r % 2 == 0:
                x.append((at(2 * chip + 1, r), at(2 * chip + 3, r)))
            else:
                x.append((at(2 * chip + 2, r), at(2 * chip + 1, r)))
    return same, next_core, x


def exchanged(x, axis, groups=None):
    return lax.all_to_all(x, axis, 0, 0, tiled=True, axis_index_groups=groups)


def projected(bands, potential, eigenvectors):
    nx, ny, nz, nb = bands.shape
    gx, gyz = lax.axis_size("gx"), lax.axis_size("gyz")
    depth = eigenvectors.shape[0]
    inner = 8
    outer = gyz // inner
    core = lax.rem(lax.axis_index("gx"), 2)
    odd = lax.rem(lax.axis_index("gyz"), 2)
    cells = nx * ny * nz
    scale = 1.0 / (cells * gyz)
    place = jnp.stack((core, odd)).astype(jnp.int32)
    pot = jnp.transpose(potential, (1, 0, 2))

    own, last, slab = prepare(place, bands, pot)
    same, next_core, x_pairs = pairs_of(gx, gyz)
    partner = [(g, g ^ 1) for g in range(gx)]
    yother = lax.ppermute(last, BOTH, next_core)
    yown = lax.ppermute(last, BOTH, same)
    other = lax.ppermute(own, "gx", partner)
    xhalo = lax.ppermute(slab, BOTH, x_pairs)
    gram = half_gram(place, own)
    gram = half_gram(place, other, (gram,))
    sent = add_cross(
        scale, inner, place, gram, own, other, yown, yother, xhalo, eigenvectors
    )
    arrived = exchanged(sent, "gyz", [[o * inner + i for i in range(inner)] for o in range(outer)])
    sent = middle(place, arrived, outer)
    arrived = exchanged(sent, "gyz", [[o * inner + i for o in range(outer)] for i in range(inner)])
    rows, coef = finish(arrived, gx, depth)
    coef_other = lax.ppermute(coef, "gx", partner)
    parts = exchanged(rows, "gx")
    sums = parts.reshape(gx // 2, 2, *parts.shape[1:]).sum(axis=0)

    left = jnp.where(core == 0, coef, coef_other)
    right = jnp.where(core == 0, coef_other, coef)
    rotated = jnp.dot(
        bands.reshape(cells, nb),
        jnp.concatenate((left, right), axis=1),
        preferred_element_type=F32,
    ).astype(BF16)
    return sums[0], sums[1], rotated.reshape(bands.shape)


def solution(mesh):
    in_specs = (P("gx", "gyz", None, None), P("gx", "gyz", None), P("gyz", None))
    out_specs = (P("gyz", None), P("gyz", None), P("gx", "gyz", None, None))
    return jax.shard_map(
        projected, mesh=mesh, in_specs=in_specs, out_specs=out_specs, check_vma=False
    )
```

```python
import functools

import jax
import jax.numpy as jnp
from jax import lax
from jax.experimental import pallas as pl
from jax.experimental.pallas import tpu as pltpu
from jax.sharding import PartitionSpec as P


F32 = jnp.float32
BF16 = jnp.bfloat16
BOTH = ("gx", "gyz")

PIECES = 3

VMEM = pl.BlockSpec(memory_space=pltpu.VMEM)
HBM = pl.BlockSpec(memory_space=pltpu.HBM)
SMEM = pl.BlockSpec(memory_space=pltpu.SMEM)


def over_rows(a, b):
    return lax.dot_general(a, b, (((0,), (0,)), ((), ())), preferred_element_type=F32)


def call(kernel, out_shape, in_specs, args, scratch=(), flops=0):
    many = isinstance(out_shape, tuple)
    moved = sum(a.size * a.dtype.itemsize for a in args)
    return pl.pallas_call(
        kernel,
        out_shape=out_shape,
        in_specs=in_specs,
        out_specs=(VMEM,) * len(out_shape) if many else VMEM,
        scratch_shapes=list(scratch),
        cost_estimate=pl.CostEstimate(flops=flops, bytes_accessed=moved, transcendentals=0),
        compiler_params=pltpu.CompilerParams(vmem_limit_bytes=10 << 20),
    )(*args)


def prepare_kernel(place_ref, bands_ref, pot_ref, held_ref, last_ref, slab_ref, pot_vmem, sems):
    nx, ny, nz, _ = bands_ref.shape
    sent = jnp.where(place_ref[1] == 0, nx - 1, 0)
    copies = (
        pltpu.make_async_copy(pot_ref, pot_vmem, sems.at[0]),
        pltpu.make_async_copy(bands_ref.at[:, ny - 1], last_ref, sems.at[1]),
        pltpu.make_async_copy(bands_ref.at[sent], slab_ref, sems.at[2]),
        pltpu.make_async_copy(bands_ref, held_ref.at[pl.ds(0, nx)], sems.at[3]),
    )
    for copy in copies:
        copy.start()
    copies[0].wait()
    rest = pot_vmem[...].reshape(nx * ny, nz)
    for piece in range(PIECES):
        part = rest.astype(BF16)
        held_ref[nx, piece, 0 : nx * ny, 0:nz] = part
        rest = rest - part.astype(F32)
    for copy in copies[1:]:
        copy.wait()


def prepare(place, bands, pot):
    nx, ny, nz, nb = bands.shape
    assert ny >= PIECES and nx * ny <= nz <= nb
    shapes = ((nx + 1, ny, nz, nb), (nx, nz, nb), (ny, nz, nb))
    bands, pot = (pltpu.with_memory_space_constraint(x, pltpu.HBM) for x in (bands, pot))
    return call(
        prepare_kernel,
        tuple(jax.ShapeDtypeStruct(s, BF16) for s in shapes),
        [SMEM, HBM, HBM],
        (place, bands, pot),
        scratch=[pltpu.VMEM(pot.shape, F32), pltpu.SemaphoreType.DMA((4,))],
    )


def half_kernel(place_ref, held_ref, *refs):
    gram_ref, right_ref, pot_ref = refs[-3:]
    nx, ny, nz, nb = right_ref.shape
    row = lax.broadcasted_iota(jnp.int32, (nz, nb), 0)

    def tiles_at(x):
        return [held_ref[x, y].astype(F32) for y in range(ny)]

    def slab(x):
        pot = jnp.transpose(pot_ref[:, pl.ds(x, 1), :].reshape(ny, nz))
        factor = 1.5 + 0.5 * pot
        tiles = tiles_at(x)
        below = None if x == 0 else tiles_at(x - 1)
        for y in range(ny):
            total = jnp.where(row > 0, pltpu.roll(tiles[y], 1, 0), 0.0)
            if y > 0:
                total += tiles[y - 1]
            if x > 0:
                total += below[y]
            right_ref[x, y] = (factor[:, y : y + 1] * tiles[y] - 0.5 * total).astype(BF16)

    def store(gram):
        gram_ref[...] = refs[0][...] + gram if len(refs) > 3 else gram

    bands = held_ref[0:nx].reshape(-1, nb)

    @pl.when(place_ref[0] == 1)
    def _():
        pieces = [held_ref[nx, p, 0 : nx * ny, 0:nz].astype(F32) for p in range(PIECES)]
        pot_ref[...] = ((pieces[2] + pieces[1]) + pieces[0]).reshape(ny, nx, nz)
        for x in range(nx):
            slab(x)
        store(over_rows(bands, right_ref[...].reshape(-1, nb)))

    @pl.when(place_ref[0] == 0)
    def _():
        store(over_rows(bands, bands))


def half_gram(place, held, given=()):
    nx, ny, nz, nb = held.shape
    nx -= 1
    return call(
        half_kernel,
        jax.ShapeDtypeStruct((nb, nb), F32),
        [SMEM] + [VMEM] * (1 + len(given)),
        (place, held, *given),
        scratch=[pltpu.VMEM((nx, ny, nz, nb), BF16), pltpu.VMEM((ny, nx, nz), F32)],
        flops=2 * nx * ny * nz * nb * nb,
    )


def cross_kernel(
    scale, place_ref, gram_ref, own_ref, other_ref, yown_ref, yother_ref, xhalo_ref, coef_ref, out_ref
):
    _, _, nb = xhalo_ref.shape
    nx = yown_ref.shape[0]
    count, depth, _ = out_ref.shape

    def rows(value):
        return value.reshape(-1, nb)

    def send(total):
        out_ref[:, :, 0:nb] = total.astype(BF16).reshape(count, depth, nb)

    coef = coef_ref[...]
    half = jnp.where(place_ref[0] == 0, coef[:, : nb // 2], coef[:, nb // 2 :])
    for target in range(count):
        out_ref[target, :, nb:] = half

    @pl.when(place_ref[0] == 1)
    def _():
        cross = over_rows(rows(own_ref[0:nx, 0]), rows(yown_ref[...]))
        cross += over_rows(rows(other_ref[0:nx, 0]), rows(yother_ref[...]))
        slab = jnp.where(place_ref[1] == 0, other_ref[0], own_ref[nx - 1])
        cross += over_rows(rows(slab), rows(xhalo_ref[...]))
        cross += over_rows(rows(own_ref[0]), rows(other_ref[nx - 1]))
        gram = gram_ref[...] - 0.5 * cross
        send(scale * (gram + jnp.transpose(gram)))

    @pl.when(place_ref[0] == 0)
    def _():
        send(scale * gram_ref[...])


def add_cross(scale, place, gram, own, other, yown, yother, xhalo, coef):
    nb = gram.shape[0]
    depth = coef.shape[0]
    halo_rows = (yown.size + yother.size + xhalo.size) // nb
    return call(
        functools.partial(cross_kernel, scale),
        jax.ShapeDtypeStruct((nb // depth, depth, nb + nb // 2), BF16),
        [SMEM] + [VMEM] * 7,
        (place, gram, own, other, yown, yother, xhalo, coef),
        flops=2 * halo_rows * nb * nb,
    )


def finish_kernel(in_ref, rows_ref, coef_ref):
    sources, _, _ = in_ref.shape
    nb = rows_ref.shape[-1]
    total = in_ref[0, :, 0:nb].astype(F32)
    for s in range(1, sources):
        total += in_ref[s, :, 0:nb].astype(F32)
    for c in range(rows_ref.shape[0]):
        rows_ref[c] = total
    coef_ref[...] = in_ref[:, :, nb:].reshape(coef_ref.shape)


def finish(arrived, copies):
    sources, depth, width = arrived.shape
    nb = sources * depth
    return call(
        finish_kernel,
        (
            jax.ShapeDtypeStruct((copies, depth, nb), F32),
            jax.ShapeDtypeStruct((nb, width - nb), BF16),
        ),
        [VMEM],
        (arrived,),
    )


def pairs_of(gx, gyz):
    def at(g, r):
        return g * gyz + r

    same, next_core, x = [], [], []
    for chip in range(gx // 2):
        for r in range(gyz - 1):
            same.append((at(2 * chip + 1, r), at(2 * chip + 1, r + 1)))
            next_core.append((at(2 * chip, r), at(2 * chip + 1, r + 1)))
    for chip in range(gx // 2 - 1):
        for r in range(gyz):
            if r % 2 == 0:
                x.append((at(2 * chip + 1, r), at(2 * chip + 3, r)))
            else:
                x.append((at(2 * chip + 2, r), at(2 * chip + 1, r)))
    return same, next_core, x


def exchanged(x, axis):
    return lax.all_to_all(x, axis, 0, 0, tiled=True)


def projected(bands, potential, eigenvectors):
    nx, ny, nz, nb = bands.shape
    gx, gyz = lax.axis_size("gx"), lax.axis_size("gyz")
    core = lax.rem(lax.axis_index("gx"), 2)
    odd = lax.rem(lax.axis_index("gyz"), 2)
    cells = nx * ny * nz
    scale = 1.0 / (cells * gyz)
    place = jnp.stack((core, odd)).astype(jnp.int32)
    pot = jnp.transpose(potential, (1, 0, 2))

    own, last, slab = prepare(place, bands, pot)
    same, next_core, x_pairs = pairs_of(gx, gyz)
    partner = [(g, g ^ 1) for g in range(gx)]
    yother = lax.ppermute(last, BOTH, next_core)
    yown = lax.ppermute(last, BOTH, same)
    other = lax.ppermute(own, "gx", partner)
    xhalo = lax.ppermute(slab, BOTH, x_pairs)
    gram = half_gram(place, own)
    gram = half_gram(place, other, (gram,))
    sent = add_cross(scale, place, gram, own, other, yown, yother, xhalo, eigenvectors)
    arrived = exchanged(sent, "gyz")
    rows, coef = finish(arrived, gx)
    coef_other = lax.ppermute(coef, "gx", partner)
    parts = exchanged(rows, "gx")
    sums = parts.reshape(gx // 2, 2, *parts.shape[1:]).sum(axis=0)

    left = jnp.where(core == 0, coef, coef_other)
    right = jnp.where(core == 0, coef_other, coef)
    rotated = jnp.dot(
        bands.reshape(cells, nb),
        jnp.concatenate((left, right), axis=1),
        preferred_element_type=F32,
    ).astype(BF16)
    return sums[0], sums[1], rotated.reshape(bands.shape)


def solution(mesh):
    in_specs = (P("gx", "gyz", None, None), P("gx", "gyz", None), P("gyz", None))
    out_specs = (P("gyz", None), P("gyz", None), P("gx", "gyz", None, None))
    return jax.shard_map(
        projected, mesh=mesh, in_specs=in_specs, out_specs=out_specs, check_vma=False
    )
```

```python
import functools

import jax
import jax.numpy as jnp
from jax import lax
from jax.experimental import pallas as pl
from jax.experimental.pallas import tpu as pltpu
from jax.sharding import PartitionSpec as P


F32 = jnp.float32
BF16 = jnp.bfloat16
BOTH = ("gx", "gyz")

PIECES = 3

VMEM = pl.BlockSpec(memory_space=pltpu.VMEM)
HBM = pl.BlockSpec(memory_space=pltpu.HBM)
SMEM = pl.BlockSpec(memory_space=pltpu.SMEM)


def over_rows(a, b):
    return lax.dot_general(a, b, (((0,), (0,)), ((), ())), preferred_element_type=F32)


def call(kernel, out_shape, in_specs, args, scratch=(), flops=0):
    many = isinstance(out_shape, tuple)
    moved = sum(a.size * a.dtype.itemsize for a in args)
    return pl.pallas_call(
        kernel,
        out_shape=out_shape,
        in_specs=in_specs,
        out_specs=(VMEM,) * len(out_shape) if many else VMEM,
        scratch_shapes=list(scratch),
        cost_estimate=pl.CostEstimate(flops=flops, bytes_accessed=moved, transcendentals=0),
        compiler_params=pltpu.CompilerParams(vmem_limit_bytes=10 << 20),
    )(*args)


def prepare_kernel(bands_ref, pot_ref, held_ref, last_ref, pot_vmem, sems):
    nx, ny, nz, _ = bands_ref.shape
    copies = (
        pltpu.make_async_copy(pot_ref, pot_vmem, sems.at[0]),
        pltpu.make_async_copy(bands_ref.at[:, ny - 1], last_ref, sems.at[1]),
        pltpu.make_async_copy(bands_ref, held_ref.at[pl.ds(0, nx)], sems.at[2]),
    )
    for copy in copies:
        copy.start()
    copies[0].wait()
    rest = pot_vmem[...].reshape(nx * ny, nz)
    for piece in range(PIECES):
        part = rest.astype(BF16)
        held_ref[nx, piece, 0 : nx * ny, 0:nz] = part
        rest = rest - part.astype(F32)
    for copy in copies[1:]:
        copy.wait()


def prepare(bands, pot):
    nx, ny, nz, nb = bands.shape
    assert ny >= PIECES and nx * ny <= nz <= nb
    shapes = ((nx + 1, ny, nz, nb), (nx, nz, nb))
    bands, pot = (pltpu.with_memory_space_constraint(x, pltpu.HBM) for x in (bands, pot))
    return call(
        prepare_kernel,
        tuple(jax.ShapeDtypeStruct(s, BF16) for s in shapes),
        [HBM, HBM],
        (bands, pot),
        scratch=[pltpu.VMEM(pot.shape, F32), pltpu.SemaphoreType.DMA((3,))],
    )


def half_kernel(place_ref, held_ref, *refs):
    gram_ref, right_ref, pot_ref = refs[-3:]
    nx, ny, nz, nb = right_ref.shape
    row = lax.broadcasted_iota(jnp.int32, (nz, nb), 0)

    def tiles_at(x):
        return [held_ref[x, y].astype(F32) for y in range(ny)]

    def slab(x):
        pot = jnp.transpose(pot_ref[:, pl.ds(x, 1), :].reshape(ny, nz))
        factor = 1.5 + 0.5 * pot
        tiles = tiles_at(x)
        below = None if x == 0 else tiles_at(x - 1)
        for y in range(ny):
            total = jnp.where(row > 0, pltpu.roll(tiles[y], 1, 0), 0.0)
            if y > 0:
                total += tiles[y - 1]
            if x > 0:
                total += below[y]
            right_ref[x, y] = (factor[:, y : y + 1] * tiles[y] - 0.5 * total).astype(BF16)

    def store(gram):
        gram_ref[...] = refs[0][...] + gram if len(refs) > 3 else gram

    bands = held_ref[0:nx].reshape(-1, nb)

    @pl.when(place_ref[0] == 1)
    def _():
        pieces = [held_ref[nx, p, 0 : nx * ny, 0:nz].astype(F32) for p in range(PIECES)]
        pot_ref[...] = ((pieces[2] + pieces[1]) + pieces[0]).reshape(ny, nx, nz)
        for x in range(nx):
            slab(x)
        store(over_rows(bands, right_ref[...].reshape(-1, nb)))

    @pl.when(place_ref[0] == 0)
    def _():
        store(over_rows(bands, bands))


def half_gram(place, held, given=()):
    nx, ny, nz, nb = held.shape
    nx -= 1
    return call(
        half_kernel,
        jax.ShapeDtypeStruct((nb, nb), F32),
        [SMEM] + [VMEM] * (1 + len(given)),
        (place, held, *given),
        scratch=[pltpu.VMEM((nx, ny, nz, nb), BF16), pltpu.VMEM((ny, nx, nz), F32)],
        flops=2 * nx * ny * nz * nb * nb,
    )


def cross_kernel(
    scale, place_ref, gram_ref, own_ref, other_ref, yown_ref, yother_ref, xhalo_ref, coef_ref, out_ref
):
    _, _, nb = xhalo_ref.shape
    nx = yown_ref.shape[0]
    count, depth, _ = out_ref.shape

    def rows(value):
        return value.reshape(-1, nb)

    def send(total):
        out_ref[:, :, 0:nb] = total.astype(BF16).reshape(count, depth, nb)

    coef = coef_ref[...]
    half = jnp.where(place_ref[0] == 0, coef[:, : nb // 2], coef[:, nb // 2 :])
    for target in range(count):
        out_ref[target, :, nb:] = half

    @pl.when(place_ref[0] == 1)
    def _():
        cross = over_rows(rows(own_ref[0:nx, 0]), rows(yown_ref[...]))
        cross += over_rows(rows(other_ref[0:nx, 0]), rows(yother_ref[...]))
        slab = jnp.where(place_ref[1] == 0, other_ref[0], own_ref[nx - 1])
        cross += over_rows(rows(slab), rows(xhalo_ref[...]))
        cross += over_rows(rows(own_ref[0]), rows(other_ref[nx - 1]))
        gram = gram_ref[...] - 0.5 * cross
        send(scale * (gram + jnp.transpose(gram)))

    @pl.when(place_ref[0] == 0)
    def _():
        send(scale * gram_ref[...])


def add_cross(scale, place, gram, own, other, yown, yother, xhalo, coef):
    nb = gram.shape[0]
    depth = coef.shape[0]
    halo_rows = (yown.size + yother.size + xhalo.size) // nb
    return call(
        functools.partial(cross_kernel, scale),
        jax.ShapeDtypeStruct((nb // depth, depth, nb + nb // 2), BF16),
        [SMEM] + [VMEM] * 7,
        (place, gram, own, other, yown, yother, xhalo, coef),
        flops=2 * halo_rows * nb * nb,
    )


def finish_kernel(in_ref, rows_ref, coef_ref):
    sources, _, _ = in_ref.shape
    nb = rows_ref.shape[-1]
    total = in_ref[0, :, 0:nb].astype(F32)
    for s in range(1, sources):
        total += in_ref[s, :, 0:nb].astype(F32)
    for c in range(rows_ref.shape[0]):
        rows_ref[c] = total
    coef_ref[...] = in_ref[:, :, nb:].reshape(coef_ref.shape)


def finish(arrived, copies):
    sources, depth, width = arrived.shape
    nb = sources * depth
    return call(
        finish_kernel,
        (
            jax.ShapeDtypeStruct((copies, depth, nb), F32),
            jax.ShapeDtypeStruct((nb, width - nb), BF16),
        ),
        [VMEM],
        (arrived,),
    )


def pairs_of(gx, gyz):
    def at(g, r):
        return g * gyz + r

    same, next_core, x = [], [], []
    for chip in range(gx // 2):
        for r in range(gyz - 1):
            same.append((at(2 * chip + 1, r), at(2 * chip + 1, r + 1)))
            next_core.append((at(2 * chip, r), at(2 * chip + 1, r + 1)))
    for chip in range(gx // 2 - 1):
        for r in range(gyz):
            if r % 2 == 0:
                x.append((at(2 * chip + 1, r), at(2 * chip + 3, r)))
            else:
                x.append((at(2 * chip + 3, r), at(2 * chip + 1, r)))
    return same, next_core, x


def exchanged(x, axis):
    return lax.all_to_all(x, axis, 0, 0, tiled=True)


def projected(bands, potential, eigenvectors):
    nx, ny, nz, nb = bands.shape
    gx, gyz = lax.axis_size("gx"), lax.axis_size("gyz")
    core = lax.rem(lax.axis_index("gx"), 2)
    odd = lax.rem(lax.axis_index("gyz"), 2)
    cells = nx * ny * nz
    scale = 1.0 / (cells * gyz)
    place = jnp.stack((core, odd)).astype(jnp.int32)
    pot = jnp.transpose(potential, (1, 0, 2))

    own, last = prepare(bands, pot)
    same, next_core, x_pairs = pairs_of(gx, gyz)
    partner = [(g, g ^ 1) for g in range(gx)]
    other = lax.ppermute(own, "gx", partner)
    yother = lax.ppermute(last, BOTH, next_core)
    yown = lax.ppermute(last, BOTH, same)
    gram = half_gram(place, own)
    slab = jnp.where(odd == 0, own[nx - 1], other[0])
    xhalo = lax.ppermute(slab, BOTH, x_pairs)
    gram = half_gram(place, other, (gram,))
    sent = add_cross(scale, place, gram, own, other, yown, yother, xhalo, eigenvectors)
    arrived = exchanged(sent, "gyz")
    rows, coef = finish(arrived, gx)
    coef_other = lax.ppermute(coef, "gx", partner)
    parts = exchanged(rows, "gx")
    sums = parts.reshape(gx // 2, 2, *parts.shape[1:]).sum(axis=0)

    left = jnp.where(core == 0, coef, coef_other)
    right = jnp.where(core == 0, coef_other, coef)
    rotated = jnp.dot(
        bands.reshape(cells, nb),
        jnp.concatenate((left, right), axis=1),
        preferred_element_type=F32,
    ).astype(BF16)
    return sums[0], sums[1], rotated.reshape(bands.shape)


def solution(mesh):
    in_specs = (P("gx", "gyz", None, None), P("gx", "gyz", None), P("gyz", None))
    out_specs = (P("gyz", None), P("gyz", None), P("gx", "gyz", None, None))
    return jax.shard_map(
        projected, mesh=mesh, in_specs=in_specs, out_specs=out_specs, check_vma=False
    )
```

```python
import functools

import jax
import jax.numpy as jnp
from jax import lax
from jax.experimental import pallas as pl
from jax.experimental.pallas import tpu as pltpu
from jax.sharding import PartitionSpec as P


F32 = jnp.float32
BF16 = jnp.bfloat16
BOTH = ("gx", "gyz")

PIECES = 3

VMEM = pl.BlockSpec(memory_space=pltpu.VMEM)
HBM = pl.BlockSpec(memory_space=pltpu.HBM)
SMEM = pl.BlockSpec(memory_space=pltpu.SMEM)


def over_rows(a, b):
    return lax.dot_general(a, b, (((0,), (0,)), ((), ())), preferred_element_type=F32)


def call(kernel, out_shape, in_specs, args, scratch=(), flops=0):
    many = isinstance(out_shape, tuple)
    moved = sum(a.size * a.dtype.itemsize for a in args)
    return pl.pallas_call(
        kernel,
        out_shape=out_shape,
        in_specs=in_specs,
        out_specs=(VMEM,) * len(out_shape) if many else VMEM,
        scratch_shapes=list(scratch),
        cost_estimate=pl.CostEstimate(flops=flops, bytes_accessed=moved, transcendentals=0),
        compiler_params=pltpu.CompilerParams(vmem_limit_bytes=10 << 20),
    )(*args)


def prepare_kernel(place_ref, bands_ref, pot_ref, held_ref, last_ref, slab_ref, pot_vmem, sems):
    nx, ny, nz, _ = bands_ref.shape
    sent = jnp.where(place_ref[1] == 0, nx - 1, 0)
    copies = (
        pltpu.make_async_copy(pot_ref, pot_vmem, sems.at[0]),
        pltpu.make_async_copy(bands_ref.at[:, ny - 1], last_ref, sems.at[1]),
        pltpu.make_async_copy(bands_ref.at[sent], slab_ref, sems.at[2]),
        pltpu.make_async_copy(bands_ref, held_ref.at[pl.ds(0, nx)], sems.at[3]),
    )
    for copy in copies:
        copy.start()
    copies[0].wait()
    rest = pot_vmem[...].reshape(nx * ny, nz)
    for piece in range(PIECES):
        part = rest.astype(BF16)
        held_ref[nx, piece, 0 : nx * ny, 0:nz] = part
        rest = rest - part.astype(F32)
    for copy in copies[1:]:
        copy.wait()


def prepare(place, bands, pot):
    nx, ny, nz, nb = bands.shape
    assert ny >= PIECES and nx * ny <= nz <= nb
    shapes = ((nx + 1, ny, nz, nb), (nx, nz, nb), (ny, nz, nb))
    bands, pot = (pltpu.with_memory_space_constraint(x, pltpu.HBM) for x in (bands, pot))
    return call(
        prepare_kernel,
        tuple(jax.ShapeDtypeStruct(s, BF16) for s in shapes),
        [SMEM, HBM, HBM],
        (place, bands, pot),
        scratch=[pltpu.VMEM(pot.shape, F32), pltpu.SemaphoreType.DMA((4,))],
    )


def half_kernel(place_ref, held_ref, *refs):
    gram_ref, right_ref, pot_ref = refs[-3:]
    nx, ny, nz, nb = right_ref.shape
    row = lax.broadcasted_iota(jnp.int32, (nz, nb), 0)

    def tiles_at(x):
        return [held_ref[x, y].astype(F32) for y in range(ny)]

    def slab(x):
        pot = jnp.transpose(pot_ref[:, pl.ds(x, 1), :].reshape(ny, nz))
        factor = 1.5 + 0.5 * pot
        tiles = tiles_at(x)
        below = None if x == 0 else tiles_at(x - 1)
        for y in range(ny):
            total = jnp.where(row > 0, pltpu.roll(tiles[y], 1, 0), 0.0)
            if y > 0:
                total += tiles[y - 1]
            if x > 0:
                total += below[y]
            right_ref[x, y] = (factor[:, y : y + 1] * tiles[y] - 0.5 * total).astype(BF16)

    def store(gram):
        gram_ref[...] = refs[0][...] + gram if len(refs) > 3 else gram

    bands = held_ref[0:nx].reshape(-1, nb)

    @pl.when(place_ref[0] == 1)
    def _():
        pieces = [held_ref[nx, p, 0 : nx * ny, 0:nz].astype(F32) for p in range(PIECES)]
        pot_ref[...] = ((pieces[2] + pieces[1]) + pieces[0]).reshape(ny, nx, nz)
        for x in range(nx):
            slab(x)
        store(over_rows(bands, right_ref[...].reshape(-1, nb)))

    @pl.when(place_ref[0] == 0)
    def _():
        store(over_rows(bands, bands))


def half_gram(place, held, given=()):
    nx, ny, nz, nb = held.shape
    nx -= 1
    return call(
        half_kernel,
        jax.ShapeDtypeStruct((nb, nb), F32),
        [SMEM] + [VMEM] * (1 + len(given)),
        (place, held, *given),
        scratch=[pltpu.VMEM((nx, ny, nz, nb), BF16), pltpu.VMEM((ny, nx, nz), F32)],
        flops=2 * nx * ny * nz * nb * nb,
    )


def pick_kernel(place_ref, last_ref, other_ref, slab_ref):
    @pl.when(place_ref[1] == 0)
    def _():
        slab_ref[...] = last_ref[...]

    @pl.when(place_ref[1] != 0)
    def _():
        slab_ref[...] = other_ref[0]


def pick(place, last, other):
    return call(
        pick_kernel,
        jax.ShapeDtypeStruct(last.shape, BF16),
        [SMEM, VMEM, VMEM],
        (place, last, other),
    )


def cross_kernel(
    scale, place_ref, gram_ref, own_ref, other_ref, yown_ref, yother_ref, xhalo_ref, out_ref
):
    _, _, nb = xhalo_ref.shape
    nx = yown_ref.shape[0]

    def rows(value):
        return value.reshape(-1, nb)

    cross = over_rows(rows(own_ref[0:nx, 0]), rows(yown_ref[...]))
    cross += over_rows(rows(other_ref[0:nx, 0]), rows(yother_ref[...]))
    slab = jnp.where(place_ref[1] == 0, other_ref[0], own_ref[nx - 1])
    cross += over_rows(rows(slab), rows(xhalo_ref[...]))
    cross += over_rows(rows(own_ref[0]), rows(other_ref[nx - 1]))
    gram = gram_ref[...] - 0.5 * cross
    out_ref[...] = (scale * (gram + jnp.transpose(gram))).astype(BF16).reshape(out_ref.shape)


def with_cross(scale, depth, place, gram, own, other, yown, yother, xhalo):
    nb = gram.shape[0]
    halo_rows = (yown.size + yother.size + xhalo.size) // nb
    return call(
        functools.partial(cross_kernel, scale),
        jax.ShapeDtypeStruct((nb // depth, depth, nb), BF16),
        [SMEM] + [VMEM] * 6,
        (place, gram, own, other, yown, yother, xhalo),
        flops=2 * halo_rows * nb * nb,
    )


def beside_kernel(scale, gram_ref, coef_ref, out_ref):
    count, depth, _ = out_ref.shape
    nb = gram_ref.shape[1]
    out_ref[:, :, 0:nb] = (scale * gram_ref[...]).astype(BF16).reshape(count, depth, nb)
    coef = coef_ref[...]
    for target in range(count):
        out_ref[target, :, nb:] = coef


def beside_coef(scale, gram, coef):
    depth, nb = coef.shape
    return call(
        functools.partial(beside_kernel, scale),
        jax.ShapeDtypeStruct((nb // depth, depth, 2 * nb), BF16),
        [VMEM] * 2,
        (gram, coef),
    )


def finish_kernel(in_ref, rows_ref, coef_ref):
    sources, _, width = in_ref.shape
    nb = rows_ref.shape[-1]
    total = in_ref[0, :, 0:nb].astype(F32)
    for s in range(1, sources):
        total += in_ref[s, :, 0:nb].astype(F32)
    for c in range(rows_ref.shape[0]):
        rows_ref[c] = total
    if width > nb:
        coef_ref[...] = in_ref[:, :, nb:].reshape(coef_ref.shape)
    else:
        coef_ref[...] = jnp.zeros(coef_ref.shape, BF16)


def finish(arrived, copies):
    sources, depth, _ = arrived.shape
    nb = sources * depth
    return call(
        finish_kernel,
        (
            jax.ShapeDtypeStruct((copies, depth, nb), F32),
            jax.ShapeDtypeStruct((nb, nb), BF16),
        ),
        [VMEM],
        (arrived,),
    )


def pairs_of(gx, gyz):
    def at(g, r):
        return g * gyz + r

    same, next_core, x = [], [], []
    for chip in range(gx // 2):
        for r in range(gyz - 1):
            same.append((at(2 * chip + 1, r), at(2 * chip + 1, r + 1)))
            next_core.append((at(2 * chip, r), at(2 * chip + 1, r + 1)))
    for chip in range(gx // 2 - 1):
        for r in range(gyz):
            if r % 2 == 0:
                x.append((at(2 * chip + 1, r), at(2 * chip + 3, r)))
            else:
                x.append((at(2 * chip + 3, r), at(2 * chip + 1, r)))
    return same, next_core, x


def exchanged(x, axis):
    return lax.all_to_all(x, axis, 0, 0, tiled=True)


def projected(bands, potential, eigenvectors):
    nx, ny, nz, nb = bands.shape
    gx, gyz = lax.axis_size("gx"), lax.axis_size("gyz")
    core = lax.rem(lax.axis_index("gx"), 2)
    odd = lax.rem(lax.axis_index("gyz"), 2)
    cells = nx * ny * nz
    scale = 1.0 / (cells * gyz)
    place = jnp.stack((core, odd)).astype(jnp.int32)
    pot = jnp.transpose(potential, (1, 0, 2))

    own, last, slab = prepare(place, bands, pot)
    same, next_core, x_pairs = pairs_of(gx, gyz)
    partner = [(g, g ^ 1) for g in range(gx)]
    yother = lax.ppermute(last, BOTH, next_core)
    yown = lax.ppermute(last, BOTH, same)
    other = lax.ppermute(own, "gx", partner)
    slab = pick(place, slab, other)
    xhalo = lax.ppermute(slab, BOTH, x_pairs)
    gram = half_gram(place, own)
    gram = half_gram(place, other, (gram,))

    def correlation_rows(*_):
        sent = beside_coef(scale, gram, eigenvectors)
        return finish(exchanged(sent, "gyz"), gx)

    def hamiltonian_rows(*halos):
        sent = with_cross(scale, eigenvectors.shape[0], place, gram, own, other, *halos)
        return finish(exchanged(sent, "gyz"), gx)

    rows, coef = lax.cond(
        core == 0, correlation_rows, hamiltonian_rows, yown, yother, xhalo
    )
    coef_other = lax.ppermute(coef, "gx", [(g, g + 1) for g in range(0, gx, 2)])
    parts = exchanged(rows, "gx")
    sums = parts.reshape(gx // 2, 2, *parts.shape[1:]).sum(axis=0)

    coef = jnp.where(core == 0, coef, coef_other)
    rotated = jnp.dot(bands.reshape(cells, nb), coef, preferred_element_type=F32).astype(BF16)
    return sums[0], sums[1], rotated.reshape(bands.shape)


def solution(mesh):
    in_specs = (P("gx", "gyz", None, None), P("gx", "gyz", None), P("gyz", None))
    out_specs = (P("gyz", None), P("gyz", None), P("gx", "gyz", None, None))
    return jax.shard_map(
        projected, mesh=mesh, in_specs=in_specs, out_specs=out_specs, check_vma=False
    )
```

```python
import functools

import jax
import jax.numpy as jnp
from jax import lax
from jax.experimental import pallas as pl
from jax.experimental.pallas import tpu as pltpu
from jax.sharding import PartitionSpec as P


F32 = jnp.float32
BF16 = jnp.bfloat16
BOTH = ("gx", "gyz")

PIECES = 3

VMEM = pl.BlockSpec(memory_space=pltpu.VMEM)
HBM = pl.BlockSpec(memory_space=pltpu.HBM)
SMEM = pl.BlockSpec(memory_space=pltpu.SMEM)


def over_rows(a, b):
    return lax.dot_general(a, b, (((0,), (0,)), ((), ())), preferred_element_type=F32)


def call(kernel, out_shape, in_specs, args, scratch=(), flops=0):
    many = isinstance(out_shape, tuple)
    moved = sum(a.size * a.dtype.itemsize for a in args)
    return pl.pallas_call(
        kernel,
        out_shape=out_shape,
        in_specs=in_specs,
        out_specs=(VMEM,) * len(out_shape) if many else VMEM,
        scratch_shapes=list(scratch),
        cost_estimate=pl.CostEstimate(flops=flops, bytes_accessed=moved, transcendentals=0),
        compiler_params=pltpu.CompilerParams(vmem_limit_bytes=10 << 20),
    )(*args)


def prepare_kernel(place_ref, bands_ref, pot_ref, held_ref, last_ref, slab_ref, pot_vmem, sems):
    nx, ny, nz, _ = bands_ref.shape
    sent = jnp.where(place_ref[1] == 0, nx - 1, 0)
    copies = (
        pltpu.make_async_copy(pot_ref, pot_vmem, sems.at[0]),
        pltpu.make_async_copy(bands_ref.at[:, ny - 1], last_ref, sems.at[1]),
        pltpu.make_async_copy(bands_ref.at[sent], slab_ref, sems.at[2]),
        pltpu.make_async_copy(bands_ref, held_ref.at[pl.ds(0, nx)], sems.at[3]),
    )
    for copy in copies:
        copy.start()
    copies[0].wait()
    rest = pot_vmem[...].reshape(nx * ny, nz)
    for piece in range(PIECES):
        part = rest.astype(BF16)
        held_ref[nx, piece, 0 : nx * ny, 0:nz] = part
        rest = rest - part.astype(F32)
    for copy in copies[1:]:
        copy.wait()


def prepare(place, bands, pot):
    nx, ny, nz, nb = bands.shape
    assert ny >= PIECES and nx * ny <= nz <= nb
    shapes = ((nx + 1, ny, nz, nb), (nx, nz, nb), (ny, nz, nb))
    bands, pot = (pltpu.with_memory_space_constraint(x, pltpu.HBM) for x in (bands, pot))
    return call(
        prepare_kernel,
        tuple(jax.ShapeDtypeStruct(s, BF16) for s in shapes),
        [SMEM, HBM, HBM],
        (place, bands, pot),
        scratch=[pltpu.VMEM(pot.shape, F32), pltpu.SemaphoreType.DMA((4,))],
    )


def half_kernel(place_ref, held_ref, *refs):
    gram_ref, right_ref, pot_ref = refs[-3:]
    nx, ny, nz, nb = right_ref.shape
    row = lax.broadcasted_iota(jnp.int32, (nz, nb), 0)

    def tiles_at(x):
        return [held_ref[x, y].astype(F32) for y in range(ny)]

    def slab(x):
        pot = jnp.transpose(pot_ref[:, pl.ds(x, 1), :].reshape(ny, nz))
        factor = 1.5 + 0.5 * pot
        tiles = tiles_at(x)
        below = None if x == 0 else tiles_at(x - 1)
        for y in range(ny):
            total = jnp.where(row > 0, pltpu.roll(tiles[y], 1, 0), 0.0)
            if y > 0:
                total += tiles[y - 1]
            if x > 0:
                total += below[y]
            right_ref[x, y] = (factor[:, y : y + 1] * tiles[y] - 0.5 * total).astype(BF16)

    def store(gram):
        gram_ref[...] = refs[0][...] + gram if len(refs) > 3 else gram

    bands = held_ref[0:nx].reshape(-1, nb)

    @pl.when(place_ref[0] == 1)
    def _():
        pieces = [held_ref[nx, p, 0 : nx * ny, 0:nz].astype(F32) for p in range(PIECES)]
        pot_ref[...] = ((pieces[2] + pieces[1]) + pieces[0]).reshape(ny, nx, nz)
        for x in range(nx):
            slab(x)
        store(over_rows(bands, right_ref[...].reshape(-1, nb)))

    @pl.when(place_ref[0] == 0)
    def _():
        store(over_rows(bands, bands))


def half_gram(place, held, given=()):
    nx, ny, nz, nb = held.shape
    nx -= 1
    return call(
        half_kernel,
        jax.ShapeDtypeStruct((nb, nb), F32),
        [SMEM] + [VMEM] * (1 + len(given)),
        (place, held, *given),
        scratch=[pltpu.VMEM((nx, ny, nz, nb), BF16), pltpu.VMEM((ny, nx, nz), F32)],
        flops=2 * nx * ny * nz * nb * nb,
    )


def pick_kernel(place_ref, last_ref, other_ref, slab_ref):
    @pl.when(place_ref[1] == 0)
    def _():
        slab_ref[...] = last_ref[...]

    @pl.when(place_ref[1] != 0)
    def _():
        slab_ref[...] = other_ref[0]


def pick(place, last, other):
    return call(
        pick_kernel,
        jax.ShapeDtypeStruct(last.shape, BF16),
        [SMEM, VMEM, VMEM],
        (place, last, other),
    )


def sides_kernel(place_ref, gram_ref, own_ref, other_ref, yown_ref, yother_ref, out_ref):
    nx, _, nb = yown_ref.shape

    def rows(value):
        return value.reshape(-1, nb)

    @pl.when(place_ref[0] == 1)
    def _():
        cross = over_rows(rows(own_ref[0:nx, 0]), rows(yown_ref[...]))
        cross += over_rows(rows(other_ref[0:nx, 0]), rows(yother_ref[...]))
        cross += over_rows(rows(own_ref[0]), rows(other_ref[nx - 1]))
        out_ref[...] = gram_ref[...] - 0.5 * cross

    @pl.when(place_ref[0] == 0)
    def _():
        out_ref[...] = gram_ref[...]


def add_sides(place, gram, own, other, yown, yother):
    nb = gram.shape[0]
    return call(
        sides_kernel,
        jax.ShapeDtypeStruct(gram.shape, F32),
        [SMEM] + [VMEM] * 5,
        (place, gram, own, other, yown, yother),
        flops=2 * (yown.size + yother.size) * nb,
    )


def cross_kernel(
    scale, place_ref, gram_ref, own_ref, other_ref, xhalo_ref, coef_ref, out_ref
):
    _, _, nb = xhalo_ref.shape
    nx = own_ref.shape[0] - 1
    count, depth, _ = out_ref.shape

    def rows(value):
        return value.reshape(-1, nb)

    def send(total):
        out_ref[:, :, 0:nb] = total.astype(BF16).reshape(count, depth, nb)

    coef = coef_ref[...]
    half = jnp.where(place_ref[0] == 0, coef[:, : nb // 2], coef[:, nb // 2 :])
    for target in range(count):
        out_ref[target, :, nb:] = half

    @pl.when(place_ref[0] == 1)
    def _():
        slab = jnp.where(place_ref[1] == 0, other_ref[0], own_ref[nx - 1])
        gram = gram_ref[...] - 0.5 * over_rows(rows(slab), rows(xhalo_ref[...]))
        send(scale * (gram + jnp.transpose(gram)))

    @pl.when(place_ref[0] == 0)
    def _():
        send(scale * gram_ref[...])


def add_cross(scale, place, gram, own, other, xhalo, coef):
    nb = gram.shape[0]
    depth = coef.shape[0]
    halo_rows = xhalo.size // nb
    return call(
        functools.partial(cross_kernel, scale),
        jax.ShapeDtypeStruct((nb // depth, depth, nb + nb // 2), BF16),
        [SMEM] + [VMEM] * 5,
        (place, gram, own, other, xhalo, coef),
        flops=2 * halo_rows * nb * nb,
    )


def finish_kernel(in_ref, rows_ref, coef_ref):
    sources, _, _ = in_ref.shape
    nb = rows_ref.shape[-1]
    total = in_ref[0, :, 0:nb].astype(F32)
    for s in range(1, sources):
        total += in_ref[s, :, 0:nb].astype(F32)
    for c in range(rows_ref.shape[0]):
        rows_ref[c] = total
    coef_ref[...] = in_ref[:, :, nb:].reshape(coef_ref.shape)


def finish(arrived, copies):
    sources, depth, width = arrived.shape
    nb = sources * depth
    return call(
        finish_kernel,
        (
            jax.ShapeDtypeStruct((copies, depth, nb), F32),
            jax.ShapeDtypeStruct((nb, width - nb), BF16),
        ),
        [VMEM],
        (arrived,),
    )


def pairs_of(gx, gyz):
    def at(g, r):
        return g * gyz + r

    same, next_core, x = [], [], []
    for chip in range(gx // 2):
        for r in range(gyz - 1):
            same.append((at(2 * chip + 1, r), at(2 * chip + 1, r + 1)))
            next_core.append((at(2 * chip, r), at(2 * chip + 1, r + 1)))
    for chip in range(gx // 2 - 1):
        for r in range(gyz):
            if r % 2 == 0:
                x.append((at(2 * chip + 1, r), at(2 * chip + 3, r)))
            else:
                x.append((at(2 * chip + 3, r), at(2 * chip + 1, r)))
    return same, next_core, x


def exchanged(x, axis):
    return lax.all_to_all(x, axis, 0, 0, tiled=True)


def projected(bands, potential, eigenvectors):
    nx, ny, nz, nb = bands.shape
    gx, gyz = lax.axis_size("gx"), lax.axis_size("gyz")
    core = lax.rem(lax.axis_index("gx"), 2)
    odd = lax.rem(lax.axis_index("gyz"), 2)
    cells = nx * ny * nz
    scale = 1.0 / (cells * gyz)
    place = jnp.stack((core, odd)).astype(jnp.int32)
    pot = jnp.transpose(potential, (1, 0, 2))

    own, last, slab = prepare(place, bands, pot)
    same, next_core, x_pairs = pairs_of(gx, gyz)
    partner = [(g, g ^ 1) for g in range(gx)]
    yother = lax.ppermute(last, BOTH, next_core)
    yown = lax.ppermute(last, BOTH, same)
    other = lax.ppermute(own, "gx", partner)
    slab = pick(place, slab, other)
    xhalo = lax.ppermute(slab, BOTH, x_pairs)
    gram = half_gram(place, own)
    gram = half_gram(place, other, (gram,))
    gram = add_sides(place, gram, own, other, yown, yother)
    sent = add_cross(scale, place, gram, own, other, xhalo, eigenvectors)
    arrived = exchanged(sent, "gyz")
    rows, coef = finish(arrived, gx)
    coef_other = lax.ppermute(coef, "gx", partner)
    parts = exchanged(rows, "gx")
    sums = parts.reshape(gx // 2, 2, *parts.shape[1:]).sum(axis=0)

    left = jnp.where(core == 0, coef, coef_other)
    right = jnp.where(core == 0, coef_other, coef)
    rotated = jnp.dot(
        bands.reshape(cells, nb),
        jnp.concatenate((left, right), axis=1),
        preferred_element_type=F32,
    ).astype(BF16)
    return sums[0], sums[1], rotated.reshape(bands.shape)


def solution(mesh):
    in_specs = (P("gx", "gyz", None, None), P("gx", "gyz", None), P("gyz", None))
    out_specs = (P("gyz", None), P("gyz", None), P("gx", "gyz", None, None))
    return jax.shard_map(
        projected, mesh=mesh, in_specs=in_specs, out_specs=out_specs, check_vma=False
    )
```

```python
import functools

import jax
import jax.numpy as jnp
from jax import lax
from jax.experimental import pallas as pl
from jax.experimental.pallas import tpu as pltpu
from jax.sharding import PartitionSpec as P


F32 = jnp.float32
BF16 = jnp.bfloat16
BOTH = ("gx", "gyz")

PIECES = 3

VMEM = pl.BlockSpec(memory_space=pltpu.VMEM)
HBM = pl.BlockSpec(memory_space=pltpu.HBM)
SMEM = pl.BlockSpec(memory_space=pltpu.SMEM)


def over_rows(a, b):
    return lax.dot_general(a, b, (((0,), (0,)), ((), ())), preferred_element_type=F32)


def call(kernel, out_shape, in_specs, args, scratch=(), flops=0):
    many = isinstance(out_shape, tuple)
    moved = sum(a.size * a.dtype.itemsize for a in args)
    return pl.pallas_call(
        kernel,
        out_shape=out_shape,
        in_specs=in_specs,
        out_specs=(VMEM,) * len(out_shape) if many else VMEM,
        scratch_shapes=list(scratch),
        cost_estimate=pl.CostEstimate(flops=flops, bytes_accessed=moved, transcendentals=0),
        compiler_params=pltpu.CompilerParams(vmem_limit_bytes=10 << 20),
    )(*args)


def prepare_kernel(place_ref, bands_ref, pot_ref, held_ref, last_ref, slab_ref, pot_vmem, sems):
    nx, ny, nz, _ = bands_ref.shape
    sent = jnp.where(place_ref[1] == 0, nx - 1, 0)
    copies = (
        pltpu.make_async_copy(pot_ref, pot_vmem, sems.at[0]),
        pltpu.make_async_copy(bands_ref.at[:, ny - 1], last_ref, sems.at[1]),
        pltpu.make_async_copy(bands_ref.at[sent], slab_ref, sems.at[2]),
        pltpu.make_async_copy(bands_ref, held_ref.at[pl.ds(0, nx)], sems.at[3]),
    )
    for copy in copies:
        copy.start()
    copies[0].wait()
    rest = pot_vmem[...].reshape(nx * ny, nz)
    for piece in range(PIECES):
        part = rest.astype(BF16)
        held_ref[nx, piece, 0 : nx * ny, 0:nz] = part
        rest = rest - part.astype(F32)
    for copy in copies[1:]:
        copy.wait()


def prepare(place, bands, pot):
    nx, ny, nz, nb = bands.shape
    assert ny >= PIECES and nx * ny <= nz <= nb
    shapes = ((nx + 1, ny, nz, nb), (nx, nz, nb), (ny, nz, nb))
    bands, pot = (pltpu.with_memory_space_constraint(x, pltpu.HBM) for x in (bands, pot))
    return call(
        prepare_kernel,
        tuple(jax.ShapeDtypeStruct(s, BF16) for s in shapes),
        [SMEM, HBM, HBM],
        (place, bands, pot),
        scratch=[pltpu.VMEM(pot.shape, F32), pltpu.SemaphoreType.DMA((4,))],
    )


def half_kernel(place_ref, held_ref, *refs):
    gram_ref, right_ref, pot_ref = refs[-3:]
    nx, ny, nz, nb = right_ref.shape
    row = lax.broadcasted_iota(jnp.int32, (nz, nb), 0)

    def tiles_at(x):
        return [held_ref[x, y].astype(F32) for y in range(ny)]

    def slab(x):
        pot = jnp.transpose(pot_ref[:, pl.ds(x, 1), :].reshape(ny, nz))
        factor = 1.5 + 0.5 * pot
        tiles = tiles_at(x)
        below = None if x == 0 else tiles_at(x - 1)
        for y in range(ny):
            total = jnp.where(row > 0, pltpu.roll(tiles[y], 1, 0), 0.0)
            if y > 0:
                total += tiles[y - 1]
            if x > 0:
                total += below[y]
            right_ref[x, y] = (factor[:, y : y + 1] * tiles[y] - 0.5 * total).astype(BF16)

    def store(gram):
        gram_ref[...] = refs[0][...] + gram if len(refs) > 3 else gram

    bands = held_ref[0:nx].reshape(-1, nb)

    @pl.when(place_ref[0] == 1)
    def _():
        pieces = [held_ref[nx, p, 0 : nx * ny, 0:nz].astype(F32) for p in range(PIECES)]
        pot_ref[...] = ((pieces[2] + pieces[1]) + pieces[0]).reshape(ny, nx, nz)
        for x in range(nx):
            slab(x)
        store(over_rows(bands, right_ref[...].reshape(-1, nb)))

    @pl.when(place_ref[0] == 0)
    def _():
        store(over_rows(bands, bands))


def half_gram(place, held, given=()):
    nx, ny, nz, nb = held.shape
    nx -= 1
    return call(
        half_kernel,
        jax.ShapeDtypeStruct((nb, nb), F32),
        [SMEM] + [VMEM] * (1 + len(given)),
        (place, held, *given),
        scratch=[pltpu.VMEM((nx, ny, nz, nb), BF16), pltpu.VMEM((ny, nx, nz), F32)],
        flops=2 * nx * ny * nz * nb * nb,
    )


def pick_kernel(place_ref, last_ref, other_ref, slab_ref):
    @pl.when(place_ref[1] == 0)
    def _():
        slab_ref[...] = last_ref[...]

    @pl.when(place_ref[1] != 0)
    def _():
        slab_ref[...] = other_ref[0]


def pick(place, last, other):
    return call(
        pick_kernel,
        jax.ShapeDtypeStruct(last.shape, BF16),
        [SMEM, VMEM, VMEM],
        (place, last, other),
    )


def cross_kernel(
    scale, place_ref, gram_ref, own_ref, other_ref, yown_ref, yother_ref, xhalo_ref, coef_ref, out_ref
):
    _, _, nb = xhalo_ref.shape
    nx = yown_ref.shape[0]
    count, depth, _ = out_ref.shape

    def rows(value):
        return value.reshape(-1, nb)

    def send(total):
        out_ref[:, :, 0:nb] = total.astype(BF16).reshape(count, depth, nb)

    coef = coef_ref[...]
    half = jnp.where(place_ref[0] == 0, coef[:, : nb // 2], coef[:, nb // 2 :])
    for target in range(count):
        out_ref[target, :, nb:] = half

    @pl.when(place_ref[0] == 1)
    def _():
        cross = over_rows(rows(own_ref[0:nx, 0]), rows(yown_ref[...]))
        cross += over_rows(rows(other_ref[0:nx, 0]), rows(yother_ref[...]))
        slab = jnp.where(place_ref[1] == 0, other_ref[0], own_ref[nx - 1])
        cross += over_rows(rows(slab), rows(xhalo_ref[...]))
        cross += over_rows(rows(own_ref[0]), rows(other_ref[nx - 1]))
        gram = gram_ref[...] - 0.5 * cross
        send(scale * (gram + jnp.transpose(gram)))

    @pl.when(place_ref[0] == 0)
    def _():
        send(scale * gram_ref[...])


def add_cross(scale, place, gram, own, other, yown, yother, xhalo, coef):
    nb = gram.shape[0]
    depth = coef.shape[0]
    halo_rows = (yown.size + yother.size + xhalo.size) // nb
    return call(
        functools.partial(cross_kernel, scale),
        jax.ShapeDtypeStruct((nb // depth, depth, nb + nb // 2), BF16),
        [SMEM] + [VMEM] * 7,
        (place, gram, own, other, yown, yother, xhalo, coef),
        flops=2 * halo_rows * nb * nb,
    )


def finish_kernel(in_ref, rows_ref, coef_ref):
    sources, _, _ = in_ref.shape
    nb = rows_ref.shape[-1]
    total = in_ref[0, :, 0:nb].astype(F32)
    for s in range(1, sources):
        total += in_ref[s, :, 0:nb].astype(F32)
    for c in range(rows_ref.shape[0]):
        rows_ref[c] = total
    coef_ref[...] = in_ref[:, :, nb:].reshape(coef_ref.shape)


def finish(arrived, copies):
    sources, depth, width = arrived.shape
    nb = sources * depth
    return call(
        finish_kernel,
        (
            jax.ShapeDtypeStruct((copies, depth, nb), F32),
            jax.ShapeDtypeStruct((nb, width - nb), BF16),
        ),
        [VMEM],
        (arrived,),
    )


def pairs_of(gx, gyz):
    def at(g, r):
        return g * gyz + r

    same, next_core, x = [], [], []
    for chip in range(gx // 2):
        for r in range(gyz - 1):
            same.append((at(2 * chip + 1, r), at(2 * chip + 1, r + 1)))
            next_core.append((at(2 * chip, r), at(2 * chip + 1, r + 1)))
    for chip in range(gx // 2 - 1):
        for r in range(gyz):
            if r % 2 == 0:
                x.append((at(2 * chip + 1, r), at(2 * chip + 3, r)))
            else:
                x.append((at(2 * chip + 3, r), at(2 * chip + 1, r)))
    return same, next_core, x


def exchanged(x, axis):
    return lax.all_to_all(x, axis, 0, 0, tiled=True)


def projected(bands, potential, eigenvectors):
    nx, ny, nz, nb = bands.shape
    gx, gyz = lax.axis_size("gx"), lax.axis_size("gyz")
    core = lax.rem(lax.axis_index("gx"), 2)
    odd = lax.rem(lax.axis_index("gyz"), 2)
    cells = nx * ny * nz
    scale = 1.0 / (cells * gyz)
    place = jnp.stack((core, odd)).astype(jnp.int32)
    pot = jnp.transpose(potential, (1, 0, 2))

    own, last, slab = prepare(place, bands, pot)
    same, next_core, x_pairs = pairs_of(gx, gyz)
    partner = [(g, g ^ 1) for g in range(gx)]
    yother = lax.ppermute(last, BOTH, next_core)
    yown = lax.ppermute(last, BOTH, same)
    other = lax.ppermute(own, "gx", partner)
    slab = pick(place, slab, other)
    xhalo = lax.ppermute(slab, BOTH, x_pairs)
    gram = half_gram(place, own)
    gram = half_gram(place, other, (gram,))
    sent = add_cross(scale, place, gram, own, other, yown, yother, xhalo, eigenvectors)
    arrived = exchanged(sent, "gyz")
    rows, coef = finish(arrived, gx)
    coef_other = lax.ppermute(coef, "gx", partner)
    parts = exchanged(rows, "gx")
    sums = parts.reshape(gx // 2, 2, *parts.shape[1:]).sum(axis=0)

    left = jnp.where(core == 0, coef, coef_other)
    right = jnp.where(core == 0, coef_other, coef)
    rotated = jnp.dot(
        bands.reshape(cells, nb),
        jnp.concatenate((left, right), axis=1),
        preferred_element_type=F32,
    ).astype(BF16)
    return sums[0], sums[1], rotated.reshape(bands.shape)


def solution(mesh):
    in_specs = (P("gx", "gyz", None, None), P("gx", "gyz", None), P("gyz", None))
    out_specs = (P("gyz", None), P("gyz", None), P("gx", "gyz", None, None))
    return jax.shard_map(
        projected, mesh=mesh, in_specs=in_specs, out_specs=out_specs, check_vma=False
    )
```
